256 devices in a mesh: node: 4 (over x), sx: 16 (over z_hi, y), sy: 4 (over z_lo, core).
Axes of the slice: x: 4, y: 4, z: 8 (z_hi: 4, z_lo: 2; z = z_hi * 2 + z_lo), core: 2. Of those that a mesh axis runs over, the one named last changes fastest.
Arguments:
- previous: float32 [4, 2, 256, 128, 256], P('node', None, 'sx', 'sy'), may hold values from 0 to 1
- feed_rate: float32 [256, 128, 256], P('sx', 'sy'), may hold values from 0.01 to 0.1
- kill_rate: float32 [256, 128, 256], P('sx', 'sy'), may hold values from 0.03 to 0.1
Outputs:
- sections: float32 [4, 2, 256, 128, 256], P('node', None, 'sx', 'sy')
The draws below stay inside these ranges and needn't reach their ends.
All inputs are finite; a program needn't handle non-finite values.
Results may differ from the reference program's by a relative error of at most 0.00011.
Values sent between devices are 32-bit elements; how exact they have to be, the bound alone decides.
A program may use at most 64 MiB of HBM per device.

```python
import math
import jax
import jax.numpy as jnp
from jax import lax

M = 4
SPECIES = 2
SWEEPS = 2
JACOBI = 12
NZ = 256
NX = 256
NY = 128


def draw_previous(key, part):
    local_key = jax.random.fold_in(key, 7301)
    first_index = jnp.arange(NX, dtype=jnp.int32)[:, None, None]
    second_index = jnp.arange(NY, dtype=jnp.int32)[None, :, None]
    third_index = jnp.arange(NZ, dtype=jnp.int32)[None, None, :]
    parity = (first_index + second_index + third_index) % 2
    pattern = (1 - 2 * parity).astype(jnp.float32)
    uniform_part = jax.random.uniform(local_key, (M, SPECIES, NX, NY, NZ), jnp.float32)
    factor = 0.5 + 0.5 * uniform_part
    values = 0.5 + 0.49 * factor * pattern[None, None]
    return values.astype(jnp.float32)


def levels(key, dims, split, least, top_value):
    def one(axis_at, parts):
        heights = jax.random.uniform(jax.random.fold_in(jax.random.fold_in(key, 6), axis_at), (parts,), jnp.float32, least / len(split), top_value / len(split))
        return jnp.repeat(jnp.exp(heights), dims[axis_at] // parts).reshape((-1,) + (1,) * (len(dims) - axis_at - 1))

    loudness = one(*split[0])
    for cut in split[1:]:
        loudness = loudness * one(*cut)
    return loudness


def setup_inputs(seed: int = 0) -> dict:
    key_of = jax.random.split(jax.random.key(seed), 4)
    previous = draw_previous(jax.random.fold_in(key_of[3], 71), 0)
    feed_rate = jnp.clip(jnp.exp(math.log(0.1) - 2.3025851 * jax.random.uniform(key_of[1], (NX, NY, NZ), jnp.float32) ** levels(key_of[1], (NX, NY, NZ), ((0, 16), (1, 4)), -0.2, 0.2)), 0.01, 0.1)
    kill_rate = jnp.clip(jnp.exp(math.log(0.1) - 1.2039728 * jax.random.uniform(key_of[2], (NX, NY, NZ), jnp.float32) ** levels(key_of[2], (NX, NY, NZ), ((0, 16), (1, 4)), -0.2, 0.2)), 0.03, 0.1)
    return {"previous": previous, "feed_rate": feed_rate, "kill_rate": kill_rate}


radau_points = [0.088587959512704, 0.409466864440735, 0.787659461760847, 1.0]
time_step = 4.0
diffusion_values = [1.0, 0.5]


def collocation():
    count = len(radau_points)
    table = []
    for row in range(count):
        table.append([0.0] * count)
    for column in range(count):
        poly = [1.0]
        denom = 1.0
        for other in range(count):
            if other != column:
                longer = [0.0] * (len(poly) + 1)
                for place in range(len(poly)):
                    longer[place + 1] = longer[place + 1] + poly[place]
                    longer[place] = longer[place] - radau_points[other] * poly[place]
                poly = longer
                denom = denom * (radau_points[column] - radau_points[other])
        for row in range(count):
            point = radau_points[row]
            total = 0.0
            for place in range(len(poly)):
                total = total + poly[place] * point ** (place + 1) / (place + 1)
            table[row][column] = total / denom
    return table


def neighbours(field):
    total = jnp.roll(field, 1, 2) + jnp.roll(field, -1, 2)
    total = total + jnp.roll(field, 1, 3) + jnp.roll(field, -1, 3)
    return total + jnp.roll(field, 1, 4) + jnp.roll(field, -1, 4)


def reaction(field, feed_rate, kill_rate):
    upart = field[:, 0]
    vpart = field[:, 1]
    uvv = upart * vpart * vpart
    first = -uvv + feed_rate[None] * (1.0 - upart)
    second = uvv - (feed_rate[None] + kill_rate[None]) * vpart
    return jnp.stack([first, second], 1)


def reference(previous, feed_rate, kill_rate):
    qmatrix = jnp.asarray(collocation(), jnp.float32)
    points = jnp.asarray(radau_points, jnp.float32)[:, None, None, None, None]
    diffusion = jnp.asarray(diffusion_values, jnp.float32)[None, :, None, None, None]
    coef = time_step * points * diffusion
    start_value = previous[-1]
    iterate = previous
    for sweep in range(SWEEPS):
        laplace = neighbours(iterate) - 6.0 * iterate
        diff = diffusion * laplace
        force = diff + reaction(iterate, feed_rate, kill_rate)
        summed = jnp.einsum("mj,jsxyz->msxyz", qmatrix, force, precision=lax.Precision.HIGHEST)
        right_side = start_value[None] + time_step * (summed - points * diff)

        def jacobi(turn, current):
            return (right_side + coef * neighbours(current)) / (1.0 + 6.0 * coef)

        iterate = lax.fori_loop(0, JACOBI, jacobi, iterate)
    return iterate
```

```python
import jax
import jax.numpy as jnp
from jax import lax
from jax.experimental import pallas as pl
from jax.experimental.pallas import tpu as pltpu
from jax.sharding import PartitionSpec as P

SWEEPS = 2
ROUNDS = 3
W = 4
NA, NB, NC = 16, 32, 256
PA, PB = NA + 2 * W, NB + 2 * W
NODES = 4
SLAB = NA // NODES
MESH = pl.DeviceIdType.MESH

radau_points = [0.088587959512704, 0.409466864440735, 0.787659461760847, 1.0]
time_step = 4.0
diffusion_values = [1.0, 0.5]


def collocation():
    count = len(radau_points)
    table = []
    for row in range(count):
        table.append([0.0] * count)
    for column in range(count):
        poly = [1.0]
        denom = 1.0
        for other in range(count):
            if other != column:
                longer = [0.0] * (len(poly) + 1)
                for place in range(len(poly)):
                    longer[place + 1] = longer[place + 1] + poly[place]
                    longer[place] = longer[place] - radau_points[other] * poly[place]
                poly = longer
                denom = denom * (radau_points[column] - radau_points[other])
        for row in range(count):
            point = radau_points[row]
            total = 0.0
            for place in range(len(poly)):
                total = total + poly[place] * point ** (place + 1) / (place + 1)
            table[row][column] = total / denom
    return table


def chosen(index, values):
    result = jnp.float32(values[-1])
    for place in range(len(values) - 2, -1, -1):
        result = jnp.where(index == place, jnp.float32(values[place]), result)
    return result


def kernel(prev, feed, kill, out, x, g, t, diff, fsend, frecv, rsend, rrecv, start,
           bsend, brecv, hs, hr, as_, ar, ss, sr):
    node = lax.axis_index("node")
    sx = lax.axis_index("sx")
    sy = lax.axis_index("sy")
    nsx = lax.axis_size("sx")
    nsy = lax.axis_size("sy")
    sx_dev = [lax.rem(sx + nsx - 1, nsx), lax.rem(sx + 1, nsx)]
    sy_dev = [lax.rem(sy + nsy - 1, nsy), lax.rem(sy + 1, nsy)]
    peers = {d: lax.rem(node + d, NODES) for d in range(NODES)}
    sources = {d: lax.rem(node + NODES - d, NODES) for d in range(NODES)}

    qmatrix = collocation()
    h_tau = chosen(node, [time_step * p for p in radau_points])
    coefs = [[time_step * p * d for p in radau_points] for d in diffusion_values]
    inv = [chosen(node, [1.0 / (1.0 + 6.0 * c) for c in cs]) for cs in coefs]
    ratio = [chosen(node, [c / (1.0 + 6.0 * c) for c in cs]) for cs in coefs]

    barrier = pltpu.get_barrier_semaphore()
    others = [{"node": peers[d]} for d in (1, 2, 3)]
    others += [{"sx": p} for p in sx_dev] + [{"sy": p} for p in sy_dev]
    for other in others:
        pl.semaphore_signal(barrier, inc=1, device_id=other, device_id_type=MESH)

    low = lax.broadcasted_iota(jnp.int32, (8, NC), 0) < W

    def loop(count, fn):
        def step(i, carry):
            fn(i)
            return carry
        lax.fori_loop(0, count, step, 0)

    def a_copy(ref, at, e, s, way, width):
        src = W if way == 0 else W + NA - width
        dst = W + NA if way == 0 else W - width
        return pltpu.make_async_remote_copy(
            src_ref=ref.at[at, s, pl.ds(src, width), pl.ds(0, NB), :],
            dst_ref=ref.at[at, s, pl.ds(dst, width), pl.ds(0, NB), :],
            send_sem=hs.at[e, s, way], recv_sem=hr.at[e, s, way],
            device_id={"sx": sx_dev[way]}, device_id_type=MESH)

    def b_copy(e, s, way, part):
        span = pl.ds(0, 8) if part == 0 else pl.ds(8, 4)
        return pltpu.make_async_remote_copy(
            src_ref=bsend.at[e, s, way, span], dst_ref=brecv.at[e, s, way, span],
            send_sem=hs.at[e, s, 2 + 2 * part + way], recv_sem=hr.at[e, s, 2 + 2 * part + way],
            device_id={"sy": sy_dev[way]}, device_id_type=MESH)

    def pair(part, p):
        return (W + p, W + 8 + p) if part == 0 else (p, W + NA + p)

    def swap(tile):
        return pltpu.roll(tile, 4, 0)

    def b_send(ref, at, e, s, part):
        base = 0 if part == 0 else 8

        def pack(p):
            one, two = pair(part, p)
            bsend[e, s, 0, base + p] = jnp.where(
                low, ref[at, s, one, 0:8, :], swap(ref[at, s, two, 0:8, :]))
            bsend[e, s, 1, base + p] = jnp.where(
                low, swap(ref[at, s, one, NB - 8:NB, :]), ref[at, s, two, NB - 8:NB, :])
        loop(8 if part == 0 else 4, pack)
        for way in range(2):
            b_copy(e, s, way, part).start()

    def b_recv(ref, at, e, s, part):
        base = 0 if part == 0 else 8
        for way in range(2):
            b_copy(e, s, way, part).wait_recv()

        def unpack(p):
            one, two = pair(part, p)
            above = brecv[e, s, 0, base + p]
            below = brecv[e, s, 1, base + p]
            ref[at, s, one, NB:PB, :] = jnp.where(low, above, swap(below))
            ref[at, s, two, NB:PB, :] = jnp.where(low, swap(above), below)
        loop(8 if part == 0 else 4, unpack)

    def halo_send(ref, at, e, s, width):
        for way in range(2):
            a_copy(ref, at, e, s, way, width).start()
        b_send(ref, at, e, s, 0)

    def a_wait(ref, at, e, s, width):
        for way in range(2):
            a_copy(ref, at, e, s, way, width).wait_recv()
        b_send(ref, at, e, s, 1)

    def f_copy(sw, s, d):
        return pltpu.make_async_remote_copy(
            src_ref=fsend.at[sw, s, peers[d]], dst_ref=frecv.at[sw, s, d - 1],
            send_sem=as_.at[sw, s, 0, d - 1], recv_sem=ar.at[sw, s, 0, d - 1],
            device_id={"node": peers[d]}, device_id_type=MESH)

    def r_copy(sw, s, d):
        return pltpu.make_async_remote_copy(
            src_ref=rsend.at[sw, s, d], dst_ref=rrecv.at[sw, s, d - 1],
            send_sem=as_.at[sw, s, 1, d - 1], recv_sem=ar.at[sw, s, 1, d - 1],
            device_id={"node": peers[d]}, device_id_type=MESH)

    def start_copy(q):
        return pltpu.make_async_remote_copy(
            src_ref=prev.at[0, :, pl.ds(SLAB * q, SLAB)], dst_ref=start,
            send_sem=ss.at[q], recv_sem=sr.at[0],
            device_id={"node": q}, device_id_type=MESH)

    def around(field):
        total = pltpu.roll(field, 1, 0) + pltpu.roll(field, PB - 1, 0)
        return total + (pltpu.roll(field, 1, 1) + pltpu.roll(field, NC - 1, 1))

    def turn(src, src_at, dst, dst_at, sw, s, first, last):
        def plane(i):
            a = first + i
            total = around(src[src_at, s, a]) + (src[src_at, s, a - 1] + src[src_at, s, a + 1])
            dst[dst_at, s, a] = g[sw, s, a] + ratio[s] * total
        loop(last - first, plane)

    def fill(a):
        for s in range(2):
            x[0, s, W + a, 0:NB, :] = prev[0, s, a]
    loop(NA, fill)
    for sw in range(SWEEPS):
        for s in range(2):
            for a in (0, PA - 1):
                g[sw, s, a] = jnp.zeros((PB, NC), jnp.float32)
    pl.semaphore_wait(barrier, len(others))
    for s in range(2):
        halo_send(x, 0, 0, s, W)

    @pl.when(node == NODES - 1)
    def _():
        for q in (1, 0, 2):
            start_copy(q).start()

        def own(a):
            for s in range(2):
                start[s, a] = prev[0, s, NA - SLAB + a]
        loop(SLAB, own)

    def sweep(sw, carry):
        e0 = ROUNDS * sw
        for s in range(2):
            a_wait(x, e0, e0, s, W)
        for s in range(2):
            b_recv(x, e0, e0, s, 0)

        def force(a):
            parts = []
            for s in range(2):
                mid = x[e0, s, W + a]
                total = around(mid)[0:NB] + (
                    x[e0, s, W + a - 1, 0:NB, :] + x[e0, s, W + a + 1, 0:NB, :])
                own = mid[0:NB]
                part = jnp.float32(diffusion_values[s]) * (total - 6.0 * own)
                diff[s, a] = part
                parts.append((own, part))
            (u, du), (v, dv) = parts
            uvv = u * v * v
            rate = feed[a]
            q = a // SLAB
            b = a % SLAB
            fsend[sw, 0, q, b] = du + (rate * (1.0 - u) - uvv)
            fsend[sw, 1, q, b] = dv + (uvv - (rate + kill[a]) * v)
        loop(NA, force)
        for s in range(2):
            for d in (2, 1, 3):
                f_copy(sw, s, d).start()

        @pl.when((sw == 0) & (node != NODES - 1))
        def _():
            start_copy(0).wait_recv()

        for s in range(2):
            for d in (1, 3, 2):
                f_copy(sw, s, d).wait_recv()

            def combine(b):
                forces = [fsend[sw, s, node, b]] + [frecv[sw, s, d - 1, b] for d in (1, 2, 3)]
                base = start[s, b]
                for d in range(NODES):
                    total = base
                    for j in range(NODES):
                        total = total + weights[d][j] * forces[j]
                    rsend[sw, s, d, b] = total
            weights = [[chosen(node, [time_step * qmatrix[(n + d) % NODES][(n - j) % NODES]
                                      for n in range(NODES)]) for j in range(NODES)]
                       for d in range(NODES)]
            loop(SLAB, combine)
            for d in (2, 1, 3):
                r_copy(sw, s, d).start()
        for s in range(2):
            b_recv(x, e0, e0, s, 1)
        for s in range(2):
            for d in (0, 1, 3, 2):
                if d:
                    r_copy(sw, s, d).wait_recv()
                q = sources[d]

                def right(b):
                    value = rsend[sw, s, 0, b] if d == 0 else rrecv[sw, s, d - 1, b]
                    a = q * SLAB + b
                    g[sw, s, W + a, 0:NB, :] = (value - h_tau * diff[s, a]) * inv[s]
                loop(SLAB, right)
            halo_send(g, sw, 2 * ROUNDS + sw, s, W - 1)
        for k in range(ROUNDS):
            e = e0 + k
            for s in range(2):
                if k == 0:
                    eg = 2 * ROUNDS + sw
                    a_wait(g, sw, eg, s, W - 1)
                    b_recv(g, sw, eg, s, 0)
                    b_recv(g, sw, eg, s, 1)
                else:
                    a_wait(x, e, e, s, W)
                    b_recv(x, e, e, s, 0)
                    b_recv(x, e, e, s, 1)
                turn(x, e, t, 0, sw, s, 1, PA - 1)
                turn(t, 0, t, 1, sw, s, 2, PA - 2)
                turn(t, 1, t, 0, sw, s, 3, PA - 3)
                turn(t, 0, x, e + 1, sw, s, 4, PA - 4)
                if k < ROUNDS - 1:
                    halo_send(x, e + 1, e + 1, s, W)
                else:
                    @pl.when(sw < SWEEPS - 1)
                    def _():
                        halo_send(x, e + 1, e + 1, s, W)
        return carry
    lax.fori_loop(0, SWEEPS, sweep, 0)

    def drain(a):
        for s in range(2):
            out[0, s, a] = x[SWEEPS * ROUNDS, s, W + a, 0:NB, :]
    loop(NA, drain)

    for e in range(2 * ROUNDS + SWEEPS):
        for s in range(2):
            for way in range(2):
                if e < 2 * ROUNDS:
                    a_copy(x, e, e, s, way, W).wait_send()
                else:
                    a_copy(g, e - 2 * ROUNDS, e, s, way, W - 1).wait_send()
                for part in range(2):
                    b_copy(e, s, way, part).wait_send()
    for sw in range(SWEEPS):
        for s in range(2):
            for d in (1, 2, 3):
                f_copy(sw, s, d).wait_send()
                r_copy(sw, s, d).wait_send()

    @pl.when(node == NODES - 1)
    def _():
        for q in range(NODES - 1):
            start_copy(q).wait_send()


def body(previous, feed_rate, kill_rate):
    f32 = jnp.float32
    exchanges = SWEEPS * (ROUNDS + 1)
    dma = pltpu.SemaphoreType.DMA
    return pl.pallas_call(
        kernel,
        out_shape=jax.ShapeDtypeStruct(previous.shape, f32),
        in_specs=[pl.BlockSpec(memory_space=pltpu.VMEM)] * 3,
        out_specs=pl.BlockSpec(memory_space=pltpu.VMEM),
        scratch_shapes=[
            pltpu.VMEM((SWEEPS * ROUNDS + 1, 2, PA, PB, NC), f32),
            pltpu.VMEM((SWEEPS, 2, PA, PB, NC), f32),
            pltpu.VMEM((2, 2, PA, PB, NC), f32),
            pltpu.VMEM((2, NA, NB, NC), f32),
            pltpu.VMEM((SWEEPS, 2, NODES, SLAB, NB, NC), f32),
            pltpu.VMEM((SWEEPS, 2, NODES - 1, SLAB, NB, NC), f32),
            pltpu.VMEM((SWEEPS, 2, NODES, SLAB, NB, NC), f32),
            pltpu.VMEM((SWEEPS, 2, NODES - 1, SLAB, NB, NC), f32),
            pltpu.VMEM((2, SLAB, NB, NC), f32),
            pltpu.VMEM((exchanges, 2, 2, 12, 8, NC), f32),
            pltpu.VMEM((exchanges, 2, 2, 12, 8, NC), f32),
            dma((exchanges, 2, 6)), dma((exchanges, 2, 6)),
            dma((SWEEPS, 2, 2, 3)), dma((SWEEPS, 2, 2, 3)),
            dma((3,)), dma((1,)),
        ],
        compiler_params=pltpu.CompilerParams(
            collective_id=0, has_side_effects=True, vmem_limit_bytes=56 * 1024 * 1024),
    )(previous, feed_rate, kill_rate)


def solution(mesh):
    return jax.shard_map(
        body,
        mesh=mesh,
        in_specs=(P("node", None, "sx", "sy", None), P("sx", "sy", None), P("sx", "sy", None)),
        out_specs=P("node", None, "sx", "sy", None),
        check_vma=False,
    )
```

```python
import jax
import jax.numpy as jnp
from jax import lax
from jax.experimental import pallas as pl
from jax.experimental.pallas import tpu as pltpu
from jax.sharding import PartitionSpec as P

SWEEPS = 2
ROUNDS = 3
W = 4
NA, NB, NC = 16, 32, 256
PA, PB = NA + 2 * W, NB + 2 * W
NODES = 4
SLAB = NA // NODES
UNROLL = 11
MESH = pl.DeviceIdType.MESH

radau_points = [0.088587959512704, 0.409466864440735, 0.787659461760847, 1.0]
time_step = 4.0
diffusion_values = [1.0, 0.5]


def collocation():
    count = len(radau_points)
    table = []
    for row in range(count):
        table.append([0.0] * count)
    for column in range(count):
        poly = [1.0]
        denom = 1.0
        for other in range(count):
            if other != column:
                longer = [0.0] * (len(poly) + 1)
                for place in range(len(poly)):
                    longer[place + 1] = longer[place + 1] + poly[place]
                    longer[place] = longer[place] - radau_points[other] * poly[place]
                poly = longer
                denom = denom * (radau_points[column] - radau_points[other])
        for row in range(count):
            point = radau_points[row]
            total = 0.0
            for place in range(len(poly)):
                total = total + poly[place] * point ** (place + 1) / (place + 1)
            table[row][column] = total / denom
    return table


def chosen(index, values):
    result = jnp.float32(values[-1])
    for place in range(len(values) - 2, -1, -1):
        result = jnp.where(index == place, jnp.float32(values[place]), result)
    return result


def kernel(prev, feed, kill, out, x, g, t0, t1, diff, fsend, frecv, rsend, rrecv, start,
           bsend, brecv, hs, hr, as_, ar, ss, sr):
    node = lax.axis_index("node")
    sx = lax.axis_index("sx")
    sy = lax.axis_index("sy")
    nsx = lax.axis_size("sx")
    nsy = lax.axis_size("sy")
    sx_dev = [lax.rem(sx + nsx - 1, nsx), lax.rem(sx + 1, nsx)]
    sy_dev = [lax.rem(sy + nsy - 1, nsy), lax.rem(sy + 1, nsy)]
    peers = {d: lax.rem(node + d, NODES) for d in range(NODES)}
    sources = {d: lax.rem(node + NODES - d, NODES) for d in range(NODES)}

    qmatrix = collocation()
    h_tau = chosen(node, [time_step * p for p in radau_points])
    coefs = [[time_step * p * d for p in radau_points] for d in diffusion_values]
    inv = [chosen(node, [1.0 / (1.0 + 6.0 * c) for c in cs]) for cs in coefs]
    ratio = [chosen(node, [c / (1.0 + 6.0 * c) for c in cs]) for cs in coefs]

    barrier = pltpu.get_barrier_semaphore()
    others = [{"node": peers[d]} for d in (1, 2, 3)]
    others += [{"sx": p} for p in sx_dev] + [{"sy": p} for p in sy_dev]
    for other in others:
        pl.semaphore_signal(barrier, inc=1, device_id=other, device_id_type=MESH)

    low = lax.broadcasted_iota(jnp.int32, (8, NC), 0) < W

    def loop(count, fn, unroll=1):
        def step(i, carry):
            for k in range(unroll):
                fn(i * unroll + k)
            return carry
        trips = count // unroll
        if trips == 1:
            step(0, 0)
        else:
            lax.fori_loop(0, trips, step, 0)
        for k in range(trips * unroll, count):
            fn(k)

    def a_copy(ref, at, e, s, way, width):
        src = W if way == 0 else W + NA - width
        dst = W + NA if way == 0 else W - width
        return pltpu.make_async_remote_copy(
            src_ref=ref.at[at, s, pl.ds(src, width), pl.ds(0, NB), :],
            dst_ref=ref.at[at, s, pl.ds(dst, width), pl.ds(0, NB), :],
            send_sem=hs.at[e, s, way], recv_sem=hr.at[e, s, way],
            device_id={"sx": sx_dev[way]}, device_id_type=MESH)

    def b_copy(e, s, way, part):
        span = pl.ds(0, 8) if part == 0 else pl.ds(8, 4)
        return pltpu.make_async_remote_copy(
            src_ref=bsend.at[e, s, way, span], dst_ref=brecv.at[e, s, way, span],
            send_sem=hs.at[e, s, 2 + 2 * part + way], recv_sem=hr.at[e, s, 2 + 2 * part + way],
            device_id={"sy": sy_dev[way]}, device_id_type=MESH)

    def pair(part, p):
        return (W + p, W + 8 + p) if part == 0 else (p, W + NA + p)

    def swap(tile):
        return pltpu.roll(tile, 4, 0)

    def b_send(ref, at, e, s, part):
        base = 0 if part == 0 else 8

        def pack(p):
            one, two = pair(part, p)
            bsend[e, s, 0, base + p] = jnp.where(
                low, ref[at, s, one, 0:8, :], swap(ref[at, s, two, 0:8, :]))
            bsend[e, s, 1, base + p] = jnp.where(
                low, swap(ref[at, s, one, NB - 8:NB, :]), ref[at, s, two, NB - 8:NB, :])
        loop(8 if part == 0 else 4, pack, 4)
        for way in range(2):
            b_copy(e, s, way, part).start()

    def b_recv(ref, at, e, s, part):
        base = 0 if part == 0 else 8
        for way in range(2):
            b_copy(e, s, way, part).wait_recv()

        def unpack(p):
            one, two = pair(part, p)
            above = brecv[e, s, 0, base + p]
            below = brecv[e, s, 1, base + p]
            ref[at, s, one, NB:PB, :] = jnp.where(low, above, swap(below))
            ref[at, s, two, NB:PB, :] = jnp.where(low, swap(above), below)
        loop(8 if part == 0 else 4, unpack, 4)

    def halo_send(ref, at, e, s, width):
        for way in range(2):
            a_copy(ref, at, e, s, way, width).start()
        b_send(ref, at, e, s, 0)

    def a_wait(ref, at, e, s, width):
        for way in range(2):
            a_copy(ref, at, e, s, way, width).wait_recv()
        b_send(ref, at, e, s, 1)

    def f_copy(sw, s, d):
        return pltpu.make_async_remote_copy(
            src_ref=fsend.at[sw, s, peers[d]], dst_ref=frecv.at[sw, s, d - 1],
            send_sem=as_.at[sw, s, 0, d - 1], recv_sem=ar.at[sw, s, 0, d - 1],
            device_id={"node": peers[d]}, device_id_type=MESH)

    def r_copy(sw, s, d):
        return pltpu.make_async_remote_copy(
            src_ref=rsend.at[sw, s, d], dst_ref=rrecv.at[sw, s, d - 1],
            send_sem=as_.at[sw, s, 1, d - 1], recv_sem=ar.at[sw, s, 1, d - 1],
            device_id={"node": peers[d]}, device_id_type=MESH)

    def start_copy(q):
        return pltpu.make_async_remote_copy(
            src_ref=prev.at[0, :, pl.ds(SLAB * q, SLAB)], dst_ref=start,
            send_sem=ss.at[q], recv_sem=sr.at[0],
            device_id={"node": q}, device_id_type=MESH)

    def around(field):
        total = pltpu.roll(field, 1, 0) + pltpu.roll(field, PB - 1, 0)
        return total + (pltpu.roll(field, 1, 1) + pltpu.roll(field, NC - 1, 1))

    def turn(src, dst, sw, s, first, last):
        def planes(i, count):
            at = [first + i + k for k in range(-1, count + 1)]
            rows = [src[a] for a in at]
            sides = [around(row) for row in rows[1:-1]]
            for k in range(count):
                total = sides[k] + (rows[k] + rows[k + 2])
                dst[at[k + 1]] = g[sw, s, at[k + 1]] + ratio[s] * total

        def step(i, carry):
            planes(i * UNROLL, UNROLL)
            return carry
        count = last - first
        trips = count // UNROLL
        lax.fori_loop(0, trips, step, 0)
        if count % UNROLL:
            planes(trips * UNROLL, count % UNROLL)

    def fill(a):
        for s in range(2):
            x[0, s, W + a, 0:NB, :] = prev[0, s, a]
    loop(NA, fill, 4)
    for sw in range(SWEEPS):
        for s in range(2):
            for a in (0, PA - 1):
                g[sw, s, a] = jnp.zeros((PB, NC), jnp.float32)
    pl.semaphore_wait(barrier, len(others))
    for s in range(2):
        halo_send(x, 0, 0, s, W)

    @pl.when(node == NODES - 1)
    def _():
        for q in (1, 0, 2):
            start_copy(q).start()

        def own(a):
            for s in range(2):
                start[s, a] = prev[0, s, NA - SLAB + a]
        loop(SLAB, own)

    def sweep(sw, carry):
        e0 = ROUNDS * sw
        for s in range(2):
            a_wait(x, e0, e0, s, W)
        for s in range(2):
            b_recv(x, e0, e0, s, 0)

        def force(a):
            parts = []
            for s in range(2):
                mid = x[e0, s, W + a]
                total = around(mid)[0:NB] + (
                    x[e0, s, W + a - 1, 0:NB, :] + x[e0, s, W + a + 1, 0:NB, :])
                own = mid[0:NB]
                part = jnp.float32(diffusion_values[s]) * (total - 6.0 * own)
                diff[s, a] = part
                parts.append((own, part))
            (u, du), (v, dv) = parts
            uvv = u * v * v
            rate = feed[a]
            q = a // SLAB
            b = a % SLAB
            fsend[sw, 0, q, b] = du + (rate * (1.0 - u) - uvv)
            fsend[sw, 1, q, b] = dv + (uvv - (rate + kill[a]) * v)
        loop(NA, force, 4)
        for s in range(2):
            for d in (2, 1, 3):
                f_copy(sw, s, d).start()

        @pl.when((sw == 0) & (node != NODES - 1))
        def _():
            start_copy(0).wait_recv()

        for s in range(2):
            for d in (1, 3, 2):
                f_copy(sw, s, d).wait_recv()

            def combine(b):
                forces = [fsend[sw, s, node, b]] + [frecv[sw, s, d - 1, b] for d in (1, 2, 3)]
                base = start[s, b]
                for d in range(NODES):
                    total = base
                    for j in range(NODES):
                        total = total + weights[d][j] * forces[j]
                    rsend[sw, s, d, b] = total
            weights = [[chosen(node, [time_step * qmatrix[(n + d) % NODES][(n - j) % NODES]
                                      for n in range(NODES)]) for j in range(NODES)]
                       for d in range(NODES)]
            loop(SLAB, combine, 2)
            for d in (2, 1, 3):
                r_copy(sw, s, d).start()
        for s in range(2):
            b_recv(x, e0, e0, s, 1)
        for s in range(2):
            for d in (0, 1, 3, 2):
                if d:
                    r_copy(sw, s, d).wait_recv()
                q = sources[d]

                def right(b):
                    value = rsend[sw, s, 0, b] if d == 0 else rrecv[sw, s, d - 1, b]
                    a = q * SLAB + b
                    g[sw, s, W + a, 0:NB, :] = (value - h_tau * diff[s, a]) * inv[s]
                loop(SLAB, right, 4)
            halo_send(g, sw, 2 * ROUNDS + sw, s, W - 1)
        for k in range(ROUNDS):
            e = e0 + k
            for s in range(2):
                if k == 0:
                    eg = 2 * ROUNDS + sw
                    a_wait(g, sw, eg, s, W - 1)
                    b_recv(g, sw, eg, s, 0)
                    b_recv(g, sw, eg, s, 1)
                else:
                    a_wait(x, e, e, s, W)
                    b_recv(x, e, e, s, 0)
                    b_recv(x, e, e, s, 1)
                turn(x.at[e, s], t0, sw, s, 1, PA - 1)
                turn(t0, t1, sw, s, 2, PA - 2)
                turn(t1, t0, sw, s, 3, PA - 3)
                turn(t0, x.at[e + 1, s], sw, s, 4, PA - 4)
                if k < ROUNDS - 1:
                    halo_send(x, e + 1, e + 1, s, W)
                else:
                    @pl.when(sw < SWEEPS - 1)
                    def _():
                        halo_send(x, e + 1, e + 1, s, W)
        return carry
    lax.fori_loop(0, SWEEPS, sweep, 0)

    def drain(a):
        for s in range(2):
            out[0, s, a] = x[SWEEPS * ROUNDS, s, W + a, 0:NB, :]
    loop(NA, drain, 4)

    for e in range(2 * ROUNDS + SWEEPS):
        for s in range(2):
            for way in range(2):
                if e < 2 * ROUNDS:
                    a_copy(x, e, e, s, way, W).wait_send()
                else:
                    a_copy(g, e - 2 * ROUNDS, e, s, way, W - 1).wait_send()
                for part in range(2):
                    b_copy(e, s, way, part).wait_send()
    for sw in range(SWEEPS):
        for s in range(2):
            for d in (1, 2, 3):
                f_copy(sw, s, d).wait_send()
                r_copy(sw, s, d).wait_send()

    @pl.when(node == NODES - 1)
    def _():
        for q in range(NODES - 1):
            start_copy(q).wait_send()


def body(previous, feed_rate, kill_rate):
    f32 = jnp.float32
    exchanges = SWEEPS * (ROUNDS + 1)
    dma = pltpu.SemaphoreType.DMA
    return pl.pallas_call(
        kernel,
        out_shape=jax.ShapeDtypeStruct(previous.shape, f32),
        in_specs=[pl.BlockSpec(memory_space=pltpu.VMEM)] * 3,
        out_specs=pl.BlockSpec(memory_space=pltpu.VMEM),
        scratch_shapes=[
            pltpu.VMEM((SWEEPS * ROUNDS + 1, 2, PA, PB, NC), f32),
            pltpu.VMEM((SWEEPS, 2, PA, PB, NC), f32),
            pltpu.VMEM((PA, PB, NC), f32),
            pltpu.VMEM((PA, PB, NC), f32),
            pltpu.VMEM((2, NA, NB, NC), f32),
            pltpu.VMEM((SWEEPS, 2, NODES, SLAB, NB, NC), f32),
            pltpu.VMEM((SWEEPS, 2, NODES - 1, SLAB, NB, NC), f32),
            pltpu.VMEM((SWEEPS, 2, NODES, SLAB, NB, NC), f32),
            pltpu.VMEM((SWEEPS, 2, NODES - 1, SLAB, NB, NC), f32),
            pltpu.VMEM((2, SLAB, NB, NC), f32),
            pltpu.VMEM((exchanges, 2, 2, 12, 8, NC), f32),
            pltpu.VMEM((exchanges, 2, 2, 12, 8, NC), f32),
            dma((exchanges, 2, 6)), dma((exchanges, 2, 6)),
            dma((SWEEPS, 2, 2, 3)), dma((SWEEPS, 2, 2, 3)),
            dma((3,)), dma((1,)),
        ],
        compiler_params=pltpu.CompilerParams(
            collective_id=0, has_side_effects=True, vmem_limit_bytes=56 * 1024 * 1024),
    )(previous, feed_rate, kill_rate)


def solution(mesh):
    return jax.shard_map(
        body,
        mesh=mesh,
        in_specs=(P("node", None, "sx", "sy", None), P("sx", "sy", None), P("sx", "sy", None)),
        out_specs=P("node", None, "sx", "sy", None),
        check_vma=False,
    )
```

```python
import jax
import jax.numpy as jnp
from jax import lax
from jax.experimental import pallas as pl
from jax.experimental.pallas import tpu as pltpu
from jax.sharding import PartitionSpec as P

SWEEPS = 2
W = 4
NA, NB, NC = 16, 32, 256
PA, PB = NA + 2 * W, NB + 2 * W
NODES = 4
SLAB = NA // NODES
XS = 3
LAST = XS * SWEEPS
MESH = pl.DeviceIdType.MESH

radau_points = [0.088587959512704, 0.409466864440735, 0.787659461760847, 1.0]
time_step = 4.0
diffusion_values = [1.0, 0.5]


def collocation():
    count = len(radau_points)
    table = []
    for row in range(count):
        table.append([0.0] * count)
    for column in range(count):
        poly = [1.0]
        denom = 1.0
        for other in range(count):
            if other != column:
                longer = [0.0] * (len(poly) + 1)
                for place in range(len(poly)):
                    longer[place + 1] = longer[place + 1] + poly[place]
                    longer[place] = longer[place] - radau_points[other] * poly[place]
                poly = longer
                denom = denom * (radau_points[column] - radau_points[other])
        for row in range(count):
            point = radau_points[row]
            total = 0.0
            for place in range(len(poly)):
                total = total + poly[place] * point ** (place + 1) / (place + 1)
            table[row][column] = total / denom
    return table


def chosen(index, values):
    result = jnp.float32(values[-1])
    for place in range(len(values) - 2, -1, -1):
        result = jnp.where(index == place, jnp.float32(values[place]), result)
    return result


def kernel(prev, feed, kill, out, x, g, t0, t1, drop, fsend, frecv, rsend, rrecv, start,
           bsend, brecv, csend, crecv, rbuf, hs, hr, as_, ar, ss, sr):
    node = lax.axis_index("node")
    sx = lax.axis_index("sx")
    sy = lax.axis_index("sy")
    nsx = lax.axis_size("sx")
    nsy = lax.axis_size("sy")
    y = lax.rem(sx, 4)
    edge = [y == 0, y == 3]
    inside = [y != 0, y != 3]
    sx_dev = [lax.rem(sx + nsx - 1, nsx), lax.rem(sx + 1, nsx)]
    in_dev = [lax.rem(sx + 3, nsx), lax.rem(sx + nsx - 3, nsx)]
    out_dev = [lax.rem(sx + nsx - 4, nsx), lax.rem(sx + 4, nsx)]
    sy_dev = [lax.rem(sy + nsy - 1, nsy), lax.rem(sy + 1, nsy)]
    peers = {d: lax.rem(node + d, NODES) for d in range(NODES)}
    sources = {d: lax.rem(node + NODES - d, NODES) for d in range(NODES)}

    qmatrix = collocation()
    coefs = [[time_step * p * d for p in radau_points] for d in diffusion_values]
    inv = [chosen(node, [1.0 / (1.0 + 6.0 * c) for c in cs]) for cs in coefs]
    ratio = [chosen(node, [c / (1.0 + 6.0 * c) for c in cs]) for cs in coefs]
    weights = [[chosen(node, [time_step * qmatrix[(n + d) % NODES][(n - j) % NODES]
                              for n in range(NODES)]) for j in range(NODES)]
               for d in range(NODES)]

    low = lax.broadcasted_iota(jnp.int32, (8, NC), 0) < 4
    barrier = pltpu.get_barrier_semaphore()
    others = [{"node": peers[d]} for d in (1, 2, 3)]
    others += [{"sx": p} for p in sx_dev + in_dev + out_dev] + [{"sy": p} for p in sy_dev]
    others += [{"sx": p, "sy": q} for p in sx_dev for q in sy_dev]
    for other in others:
        pl.semaphore_signal(barrier, inc=1, device_id=other, device_id_type=MESH)

    def loop(count, fn, unroll=1):
        def step(i, carry):
            for k in range(unroll):
                fn(i * unroll + k)
            return carry
        lax.fori_loop(0, count // unroll, step, 0)

    def remote(src, dst, e, s, slot, device):
        return pltpu.make_async_remote_copy(
            src_ref=src, dst_ref=dst, send_sem=hs.at[e, s, slot], recv_sem=hr.at[e, s, slot],
            device_id=device, device_id_type=MESH)

    def span(way, first, last):
        if way == 0:
            return W + first - 1, W + NA + first - 1, last - first + 1
        return W + NA - last, W - last, last - first + 1

    def relayed(ex):
        return (ex[4] - ex[3] + 1) // 2

    def a_copy(ex, s, way, first, last, slot):
        ref, at, e = ex[:3]
        src, dst, count = span(way, first, last)
        return remote(ref.at[at, s, pl.ds(src, count), pl.ds(0, NB), :],
                      ref.at[at, s, pl.ds(dst, count), pl.ds(0, NB), :],
                      e, s, slot + way, {"sx": sx_dev[way]})

    def relay_in(ex, s, way):
        ref, at, e, first, last = ex
        src, dst, count = span(way, last - relayed(ex) + 1, last)
        return remote(ref.at[at, s, pl.ds(src, count), pl.ds(0, NB), :],
                      rbuf.at[e, s, pl.ds(0, count)], e, s, 2, {"sx": in_dev[way]})

    def relay_out(ex, s, way):
        ref, at, e, first, last = ex
        src, dst, count = span(way, last - relayed(ex) + 1, last)
        return remote(rbuf.at[e, s, pl.ds(0, count)],
                      ref.at[at, s, pl.ds(dst, count), pl.ds(0, NB), :],
                      e, s, 3, {"sx": out_dev[way]})

    def whole(ex, s, way):
        return a_copy(ex, s, way, ex[3], ex[4], 0)

    def direct(ex, s, way):
        return a_copy(ex, s, way, ex[3], ex[4] - relayed(ex), 0)

    def layer(ex, s, way):
        return a_copy(ex, s, way, 1, 1, 10)

    def b_copy(ex, s, way):
        e = ex[2]
        return remote(bsend.at[e, s, way], brecv.at[e, s, way],
                      e, s, 4 + way, {"sy": sy_dev[way]})

    def c_copy(ex, s, n):
        e = ex[2]
        return remote(csend.at[e, s, n], crecv.at[e, s, n],
                      e, s, 6 + n, {"sx": sx_dev[n // 2], "sy": sy_dev[n % 2]})

    def swap(tile):
        return pltpu.roll(tile, 4, 0)

    def first_rows(ex, s, one, two):
        ref, at = ex[:2]
        return jnp.where(low, ref[at, s, one, 0:8, :], swap(ref[at, s, two, 0:8, :]))

    def last_rows(ex, s, one, two):
        ref, at = ex[:2]
        return jnp.where(low, swap(ref[at, s, one, NB - 8:NB, :]), ref[at, s, two, NB - 8:NB, :])

    def put_rows(ex, s, one, two, above, below):
        ref, at = ex[:2]
        ref[at, s, one, NB:PB, :] = jnp.where(low, above, swap(below))
        ref[at, s, two, NB:PB, :] = jnp.where(low, swap(above), below)

    def b_send(ex, s):
        e = ex[2]

        def pack(p):
            bsend[e, s, 0, p] = first_rows(ex, s, W + p, W + 8 + p)
            bsend[e, s, 1, p] = last_rows(ex, s, W + p, W + 8 + p)
        loop(8, pack, 4)
        for way in range(2):
            b_copy(ex, s, way).start()

    def b_recv(ex, s):
        e = ex[2]
        for way in range(2):
            b_copy(ex, s, way).wait_recv()

        def unpack(p):
            put_rows(ex, s, W + p, W + 8 + p, brecv[e, s, 0, p], brecv[e, s, 1, p])
        loop(8, unpack, 4)

    def c_send(ex, s):
        e = ex[2]
        for n in range(4):
            base = W if n < 2 else NA
            for p in range(2):
                rows = first_rows if n % 2 == 0 else last_rows
                csend[e, s, n, p] = rows(ex, s, base + p, base + p + 2)
            c_copy(ex, s, n).start()

    def c_recv(ex, s):
        e = ex[2]
        for n in range(4):
            c_copy(ex, s, n).wait_recv()
        for way in range(2):
            base = W + NA if way == 0 else 0
            for p in range(2):
                put_rows(ex, s, base + p, base + p + 2,
                         crecv[e, s, 2 * way, p], crecv[e, s, 2 * way + 1, p])

    def relay(ex, s):
        for way in range(2):
            @pl.when(edge[1 - way])
            def _():
                relay_in(ex, s, way).wait_recv()
                relay_out(ex, s, way).start()

    def halo_send(ex, s):
        if ex[3] > 1:
            for way in range(2):
                layer(ex, s, way).start()
            b_send(ex, s)
        for way in range(2):
            @pl.when(edge[way])
            def _():
                relay_in(ex, s, way).start()
                direct(ex, s, way).start()

            @pl.when(inside[way])
            def _():
                whole(ex, s, way).start()
        c_send(ex, s)
        if ex[3] == 1:
            b_send(ex, s)

    def near_wait(ex, s):
        for way in range(2):
            layer(ex, s, way).wait_recv()
        b_recv(ex, s)

    def a_wait(ex, s):
        for way in range(2):
            @pl.when(edge[1 - way])
            def _():
                direct(ex, s, way).wait_recv()
                relay_out(ex, s, way).wait_recv()

            @pl.when(inside[1 - way])
            def _():
                whole(ex, s, way).wait_recv()

    def b_wait(ex, s):
        if ex[3] == 1:
            b_recv(ex, s)
        c_recv(ex, s)

    def sent(ex, s):
        for way in range(2):
            if ex[3] > 1:
                layer(ex, s, way).wait_send()

            @pl.when(edge[way])
            def _():
                relay_in(ex, s, way).wait_send()
                direct(ex, s, way).wait_send()

            @pl.when(inside[way])
            def _():
                whole(ex, s, way).wait_send()

            @pl.when(edge[1 - way])
            def _():
                relay_out(ex, s, way).wait_send()
        for way in range(2):
            b_copy(ex, s, way).wait_send()
        for n in range(4):
            c_copy(ex, s, n).wait_send()

    def f_copy(sw, s, d):
        return pltpu.make_async_remote_copy(
            src_ref=fsend.at[sw, s, peers[d]], dst_ref=frecv.at[sw, s, d - 1],
            send_sem=as_.at[sw, s, 0, d - 1], recv_sem=ar.at[sw, s, 0, d - 1],
            device_id={"node": peers[d]}, device_id_type=MESH)

    def r_copy(sw, s, d):
        return pltpu.make_async_remote_copy(
            src_ref=rsend.at[sw, s, d], dst_ref=rrecv.at[sw, s, d - 1],
            send_sem=as_.at[sw, s, 1, d - 1], recv_sem=ar.at[sw, s, 1, d - 1],
            device_id={"node": peers[d]}, device_id_type=MESH)

    def start_copy(q):
        return pltpu.make_async_remote_copy(
            src_ref=prev.at[0, :, pl.ds(SLAB * q, SLAB)], dst_ref=start,
            send_sem=ss.at[q], recv_sem=sr.at[0],
            device_id={"node": q}, device_id_type=MESH)

    def around(field):
        total = pltpu.roll(field, 1, 0) + pltpu.roll(field, PB - 1, 0)
        return total + (pltpu.roll(field, 1, 1) + pltpu.roll(field, NC - 1, 1))

    def turn(src, dst, sw, s, level, rows=PB):
        half = (PA - 2 * level) // 2

        def step(i, carry):
            at = [level + i * half + k for k in range(-1, half + 1)]
            planes = [src[a] for a in at]
            sides = [around(plane)[0:rows] for plane in planes[1:-1]]
            for k in range(half):
                total = sides[k] + (planes[k][0:rows] + planes[k + 2][0:rows])
                dst[at[k + 1], 0:rows, :] = g[sw, s, at[k + 1], 0:rows, :] + ratio[s] * total
            return carry
        lax.fori_loop(0, 2, step, 0)

    def fill(a):
        for s in range(2):
            x[0, s, W + a, 0:NB, :] = prev[0, s, a]
    loop(NA, fill, 4)
    for sw in range(SWEEPS):
        for s in range(2):
            for a in (0, PA - 1):
                g[sw, s, a] = jnp.zeros((PB, NC), jnp.float32)
    pl.semaphore_wait(barrier, len(others))
    for s in range(2):
        halo_send((x, 0, 0, 2, W), s)

    @pl.when(node == NODES - 1)
    def _():
        for q in (1, 0, 2):
            start_copy(q).start()

        def own(a):
            for s in range(2):
                start[s, a] = prev[0, s, NA - SLAB + a]
        loop(SLAB, own, 4)

    def sweep(sw, carry):
        e0 = XS * sw
        ex_0 = (x, e0, e0, 2, W)
        exs = [ex_0] + [(x, e0 + k, e0 + k, 1, W) for k in range(1, XS)]
        exs += [(x, e0 + XS, e0 + XS, 2, W)]
        ex_g = (g, sw, LAST + sw, 1, W - 1)
        for s in range(2):
            near_wait(ex_0, s)

        def force(a):
            parts = []
            for s in range(2):
                mid = x[e0, s, W + a]
                total = around(mid)[0:NB] + (
                    x[e0, s, W + a - 1, 0:NB, :] + x[e0, s, W + a + 1, 0:NB, :])
                own = mid[0:NB]
                gap = total - 6.0 * own
                drop[s, a] = ratio[s] * gap
                parts.append((own, jnp.float32(diffusion_values[s]) * gap))
            (u, du), (v, dv) = parts
            uvv = u * v * v
            rate = feed[a]
            return du + (rate * (1.0 - u) - uvv), dv + (uvv - (rate + kill[a]) * v)

        for d in (2, 1, 3, 0):
            def slab(b):
                pair = force(peers[d] * SLAB + b)
                for s in range(2):
                    fsend[sw, s, peers[d], b] = pair[s]
            loop(SLAB, slab, 4)
            if d:
                f_copy(sw, 0, d).start()
        for d in (2, 1, 3):
            f_copy(sw, 1, d).start()

        for s in range(2):
            relay(ex_0, s)

        @pl.when((sw == 0) & (node != NODES - 1))
        def _():
            start_copy(0).wait_recv()

        for s in range(2):
            for d in (1, 3, 2):
                f_copy(sw, s, d).wait_recv()

            def combine(b):
                forces = [fsend[sw, s, node, b]] + [frecv[sw, s, d - 1, b] for d in (1, 2, 3)]
                base = start[s, b]
                for d in range(NODES):
                    total = base
                    for j in range(NODES):
                        total = total + weights[d][j] * forces[j]
                    rsend[sw, s, d, b] = total
            loop(SLAB, combine, 2)
            for d in (2, 1, 3):
                r_copy(sw, s, d).start()

        for s in range(2):
            a_wait(ex_0, s)
        for s in range(2):
            for d in (0, 1, 3, 2):
                if d:
                    r_copy(sw, s, d).wait_recv()
                q = sources[d]

                def right(b):
                    value = rsend[sw, s, 0, b] if d == 0 else rrecv[sw, s, d - 1, b]
                    a = q * SLAB + b
                    g[sw, s, W + a, 0:NB, :] = value * inv[s] - drop[s, a]
                loop(SLAB, right, 4)
            halo_send(ex_g, s)
        for s in range(2):
            relay(ex_g, s)

        for k in range(XS):
            now = ex_g if k == 0 else exs[k]
            for s in range(2):
                a_wait(now, s)
                if s == 0 and k > 0:
                    relay(now, 1)
                if s == 1 and k < XS - 1:
                    relay(exs[k + 1], 0)
                b_wait(now, s)
                if k == 0:
                    b_wait(ex_0, s)
                turn(x.at[e0 + k, s], t0, sw, s, 1)
                turn(t0, t1, sw, s, 2)
                turn(t1, t0, sw, s, 3)
                turn(t0, x.at[e0 + k + 1, s], sw, s, 4, NB)
                if k < XS - 1:
                    halo_send(exs[k + 1], s)
                else:
                    @pl.when(sw < SWEEPS - 1)
                    def _():
                        halo_send(exs[XS], s)
        return carry
    lax.fori_loop(0, SWEEPS, sweep, 0)

    def drain(a):
        for s in range(2):
            out[0, s, a] = x[LAST, s, W + a, 0:NB, :]
    loop(NA, drain, 4)

    for s in range(2):
        for sw in range(SWEEPS):
            sent((g, sw, LAST + sw, 1, W - 1), s)
            sent((x, XS * sw, XS * sw, 2, W), s)
            for k in range(1, XS):
                sent((x, XS * sw + k, XS * sw + k, 1, W), s)
            for d in (1, 2, 3):
                f_copy(sw, s, d).wait_send()
                r_copy(sw, s, d).wait_send()

    @pl.when(node == NODES - 1)
    def _():
        for q in range(NODES - 1):
            start_copy(q).wait_send()


def body(previous, feed_rate, kill_rate):
    f32 = jnp.float32
    exchanges = LAST + SWEEPS
    dma = pltpu.SemaphoreType.DMA
    return pl.pallas_call(
        kernel,
        out_shape=jax.ShapeDtypeStruct(previous.shape, f32),
        in_specs=[pl.BlockSpec(memory_space=pltpu.VMEM)] * 3,
        out_specs=pl.BlockSpec(memory_space=pltpu.VMEM),
        scratch_shapes=[
            pltpu.VMEM((LAST + 1, 2, PA, PB, NC), f32),
            pltpu.VMEM((SWEEPS, 2, PA, PB, NC), f32),
            pltpu.VMEM((PA, PB, NC), f32),
            pltpu.VMEM((PA, PB, NC), f32),
            pltpu.VMEM((2, NA, NB, NC), f32),
            pltpu.VMEM((SWEEPS, 2, NODES, SLAB, NB, NC), f32),
            pltpu.VMEM((SWEEPS, 2, NODES - 1, SLAB, NB, NC), f32),
            pltpu.VMEM((SWEEPS, 2, NODES, SLAB, NB, NC), f32),
            pltpu.VMEM((SWEEPS, 2, NODES - 1, SLAB, NB, NC), f32),
            pltpu.VMEM((2, SLAB, NB, NC), f32),
            pltpu.VMEM((exchanges, 2, 2, 8, 8, NC), f32),
            pltpu.VMEM((exchanges, 2, 2, 8, 8, NC), f32),
            pltpu.VMEM((exchanges, 2, 4, 2, 8, NC), f32),
            pltpu.VMEM((exchanges, 2, 4, 2, 8, NC), f32),
            pltpu.VMEM((exchanges, 2, W // 2, NB, NC), f32),
            dma((exchanges, 2, 12)), dma((exchanges, 2, 12)),
            dma((SWEEPS, 2, 2, 3)), dma((SWEEPS, 2, 2, 3)),
            dma((3,)), dma((1,)),
        ],
        compiler_params=pltpu.CompilerParams(
            collective_id=0, has_side_effects=True, vmem_limit_bytes=56 * 1024 * 1024),
    )(previous, feed_rate, kill_rate)


def solution(mesh):
    return jax.shard_map(
        body,
        mesh=mesh,
        in_specs=(P("node", None, "sx", "sy", None), P("sx", "sy", None), P("sx", "sy", None)),
        out_specs=P("node", None, "sx", "sy", None),
        check_vma=False,
    )
```

```python
import jax
import jax.numpy as jnp
from jax import lax
from jax.experimental import pallas as pl
from jax.experimental.pallas import tpu as pltpu
from jax.sharding import PartitionSpec as P

SWEEPS = 2
W = 4
NA, NB, NC = 16, 32, 256
PA, PB = NA + 2 * W, NB + 2 * W
NODES = 4
SLAB = NA // NODES
XS = 3
LAST = XS * SWEEPS
MESH = pl.DeviceIdType.MESH

radau_points = [0.088587959512704, 0.409466864440735, 0.787659461760847, 1.0]
time_step = 4.0
diffusion_values = [1.0, 0.5]


def collocation():
    count = len(radau_points)
    table = []
    for row in range(count):
        table.append([0.0] * count)
    for column in range(count):
        poly = [1.0]
        denom = 1.0
        for other in range(count):
            if other != column:
                longer = [0.0] * (len(poly) + 1)
                for place in range(len(poly)):
                    longer[place + 1] = longer[place + 1] + poly[place]
                    longer[place] = longer[place] - radau_points[other] * poly[place]
                poly = longer
                denom = denom * (radau_points[column] - radau_points[other])
        for row in range(count):
            point = radau_points[row]
            total = 0.0
            for place in range(len(poly)):
                total = total + poly[place] * point ** (place + 1) / (place + 1)
            table[row][column] = total / denom
    return table


def chosen(index, values):
    result = jnp.float32(values[-1])
    for place in range(len(values) - 2, -1, -1):
        result = jnp.where(index == place, jnp.float32(values[place]), result)
    return result


def kernel(prev, feed, kill, out, x, g, t0, t1, drop, fsend, frecv, rsend, rrecv, start,
           bsend, brecv, csend, crecv, rbuf, hs, hr, as_, ar, ss, sr):
    node = lax.axis_index("node")
    sx = lax.axis_index("sx")
    sy = lax.axis_index("sy")
    nsx = lax.axis_size("sx")
    nsy = lax.axis_size("sy")
    y = lax.rem(sx, 4)
    edge = [y == 0, y == 3]
    inside = [y != 0, y != 3]
    sx_dev = [lax.rem(sx + nsx - 1, nsx), lax.rem(sx + 1, nsx)]
    in_dev = [lax.rem(sx + 3, nsx), lax.rem(sx + nsx - 3, nsx)]
    out_dev = [lax.rem(sx + nsx - 4, nsx), lax.rem(sx + 4, nsx)]
    sy_dev = [lax.rem(sy + nsy - 1, nsy), lax.rem(sy + 1, nsy)]
    peers = {d: lax.rem(node + d, NODES) for d in range(NODES)}
    sources = {d: lax.rem(node + NODES - d, NODES) for d in range(NODES)}

    qmatrix = collocation()
    coefs = [[time_step * p * d for p in radau_points] for d in diffusion_values]
    inv = [chosen(node, [1.0 / (1.0 + 6.0 * c) for c in cs]) for cs in coefs]
    ratio = [chosen(node, [c / (1.0 + 6.0 * c) for c in cs]) for cs in coefs]
    weights = [[chosen(node, [time_step * qmatrix[(n + d) % NODES][(n - j) % NODES]
                              for n in range(NODES)]) for j in range(NODES)]
               for d in range(NODES)]

    low = lax.broadcasted_iota(jnp.int32, (8, NC), 0) < 4
    barrier = pltpu.get_barrier_semaphore()
    others = [{"node": peers[d]} for d in (1, 2, 3)]
    others += [{"sx": p} for p in sx_dev + in_dev + out_dev] + [{"sy": p} for p in sy_dev]
    others += [{"sx": p, "sy": q} for p in sx_dev for q in sy_dev]
    for other in others:
        pl.semaphore_signal(barrier, inc=1, device_id=other, device_id_type=MESH)

    def loop(count, fn, unroll=1):
        def step(i, carry):
            for k in range(unroll):
                fn(i * unroll + k)
            return carry
        lax.fori_loop(0, count // unroll, step, 0)

    def remote(src, dst, e, s, slot, device):
        return pltpu.make_async_remote_copy(
            src_ref=src, dst_ref=dst, send_sem=hs.at[e, s, slot], recv_sem=hr.at[e, s, slot],
            device_id=device, device_id_type=MESH)

    def span(way, first, last):
        if way == 0:
            return W + first - 1, W + NA + first - 1, last - first + 1
        return W + NA - last, W - last, last - first + 1

    def relayed(ex):
        return 2

    def a_copy(ex, s, way, first, last, slot):
        ref, at, e = ex[:3]
        src, dst, count = span(way, first, last)
        return remote(ref.at[at, s, pl.ds(src, count), pl.ds(0, NB), :],
                      ref.at[at, s, pl.ds(dst, count), pl.ds(0, NB), :],
                      e, s, slot + way, {"sx": sx_dev[way]})

    def relay_in(ex, s, way):
        ref, at, e, first, last = ex
        src, dst, count = span(way, last - relayed(ex) + 1, last)
        return remote(ref.at[at, s, pl.ds(src, count), pl.ds(0, NB), :],
                      rbuf.at[e, s, pl.ds(0, count)], e, s, 2, {"sx": in_dev[way]})

    def relay_out(ex, s, way):
        ref, at, e, first, last = ex
        src, dst, count = span(way, last - relayed(ex) + 1, last)
        return remote(rbuf.at[e, s, pl.ds(0, count)],
                      ref.at[at, s, pl.ds(dst, count), pl.ds(0, NB), :],
                      e, s, 3, {"sx": out_dev[way]})

    def whole(ex, s, way):
        return a_copy(ex, s, way, ex[3], ex[4], 0)

    def direct(ex, s, way):
        return a_copy(ex, s, way, ex[3], ex[4] - relayed(ex), 0)

    def layer(ex, s, way):
        return a_copy(ex, s, way, 1, 1, 10)

    def b_copy(ex, s, way):
        e = ex[2]
        return remote(bsend.at[e, s, way], brecv.at[e, s, way],
                      e, s, 4 + way, {"sy": sy_dev[way]})

    def c_copy(ex, s, n):
        e = ex[2]
        return remote(csend.at[e, s, n], crecv.at[e, s, n],
                      e, s, 6 + n, {"sx": sx_dev[n // 2], "sy": sy_dev[n % 2]})

    def swap(tile):
        return pltpu.roll(tile, 4, 0)

    def first_rows(ex, s, one, two):
        ref, at = ex[:2]
        return jnp.where(low, ref[at, s, one, 0:8, :], swap(ref[at, s, two, 0:8, :]))

    def last_rows(ex, s, one, two):
        ref, at = ex[:2]
        return jnp.where(low, swap(ref[at, s, one, NB - 8:NB, :]), ref[at, s, two, NB - 8:NB, :])

    def put_rows(ex, s, one, two, above, below):
        ref, at = ex[:2]
        ref[at, s, one, NB:PB, :] = jnp.where(low, above, swap(below))
        ref[at, s, two, NB:PB, :] = jnp.where(low, swap(above), below)

    def b_send(ex, s):
        e = ex[2]

        def pack(p):
            bsend[e, s, 0, p] = first_rows(ex, s, W + p, W + 8 + p)
            bsend[e, s, 1, p] = last_rows(ex, s, W + p, W + 8 + p)
        loop(8, pack, 4)
        for way in range(2):
            b_copy(ex, s, way).start()

    def b_recv(ex, s):
        e = ex[2]
        for way in range(2):
            b_copy(ex, s, way).wait_recv()

        def unpack(p):
            put_rows(ex, s, W + p, W + 8 + p, brecv[e, s, 0, p], brecv[e, s, 1, p])
        loop(8, unpack, 4)

    def c_send(ex, s):
        e = ex[2]
        for n in range(4):
            base = W if n < 2 else NA
            for p in range(2):
                rows = first_rows if n % 2 == 0 else last_rows
                csend[e, s, n, p] = rows(ex, s, base + p, base + p + 2)
            c_copy(ex, s, n).start()

    def c_recv(ex, s):
        e = ex[2]
        for n in range(4):
            c_copy(ex, s, n).wait_recv()
        for way in range(2):
            base = W + NA if way == 0 else 0
            for p in range(2):
                put_rows(ex, s, base + p, base + p + 2,
                         crecv[e, s, 2 * way, p], crecv[e, s, 2 * way + 1, p])

    def relay(ex, s):
        for way in range(2):
            @pl.when(edge[1 - way])
            def _():
                relay_in(ex, s, way).wait_recv()
                relay_out(ex, s, way).start()

    def halo_send(ex, s):
        if ex[3] > 1:
            for way in range(2):
                layer(ex, s, way).start()
            b_send(ex, s)
        for way in range(2):
            @pl.when(edge[way])
            def _():
                relay_in(ex, s, way).start()
                direct(ex, s, way).start()

            @pl.when(inside[way])
            def _():
                whole(ex, s, way).start()
        c_send(ex, s)
        if ex[3] == 1:
            b_send(ex, s)

    def near_wait(ex, s):
        for way in range(2):
            layer(ex, s, way).wait_recv()
        b_recv(ex, s)

    def a_wait(ex, s):
        for way in range(2):
            @pl.when(edge[1 - way])
            def _():
                direct(ex, s, way).wait_recv()
                relay_out(ex, s, way).wait_recv()

            @pl.when(inside[1 - way])
            def _():
                whole(ex, s, way).wait_recv()

    def sent(ex, s):
        for way in range(2):
            if ex[3] > 1:
                layer(ex, s, way).wait_send()

            @pl.when(edge[way])
            def _():
                relay_in(ex, s, way).wait_send()
                direct(ex, s, way).wait_send()

            @pl.when(inside[way])
            def _():
                whole(ex, s, way).wait_send()

            @pl.when(edge[1 - way])
            def _():
                relay_out(ex, s, way).wait_send()
        for way in range(2):
            b_copy(ex, s, way).wait_send()
        for n in range(4):
            c_copy(ex, s, n).wait_send()

    def f_copy(sw, s, d):
        return pltpu.make_async_remote_copy(
            src_ref=fsend.at[sw, s, peers[d]], dst_ref=frecv.at[sw, s, d - 1],
            send_sem=as_.at[sw, s, 0, d - 1], recv_sem=ar.at[sw, s, 0, d - 1],
            device_id={"node": peers[d]}, device_id_type=MESH)

    def r_copy(sw, s, d):
        return pltpu.make_async_remote_copy(
            src_ref=rsend.at[sw, s, d], dst_ref=rrecv.at[sw, s, d - 1],
            send_sem=as_.at[sw, s, 1, d - 1], recv_sem=ar.at[sw, s, 1, d - 1],
            device_id={"node": peers[d]}, device_id_type=MESH)

    def start_copy(q):
        return pltpu.make_async_remote_copy(
            src_ref=prev.at[0, :, pl.ds(SLAB * q, SLAB)], dst_ref=start,
            send_sem=ss.at[q], recv_sem=sr.at[0],
            device_id={"node": q}, device_id_type=MESH)

    def around(field):
        total = pltpu.roll(field, 1, 0) + pltpu.roll(field, PB - 1, 0)
        return total + (pltpu.roll(field, 1, 1) + pltpu.roll(field, NC - 1, 1))

    def advance(src, dst, sw, s, base, groups, rows):
        held = {}
        for first, count in groups:
            for a in range(first - 1, first + count + 1):
                if a not in held:
                    held[a] = src[base + a]
        sides = {a: around(held[a])[0:rows] for first, count in groups
                 for a in range(first, first + count)}
        for a, side in sides.items():
            total = side + (held[a - 1][0:rows] + held[a + 1][0:rows])
            dst[base + a, 0:rows, :] = g[sw, s, base + a, 0:rows, :] + ratio[s] * total

    def inner(src, dst, sw, s, level, rows=PB):
        half = NA // 2 - level

        def step(i, carry):
            advance(src, dst, sw, s, W + level + i * half, [(0, half)], rows)
            return carry
        lax.fori_loop(0, 2, step, 0)

    def outer(src, dst, sw, s, level, rows=PB):
        advance(src, dst, sw, s, 0, [(level, W), (PA - W - level, W)], rows)

    def fill(a):
        for s in range(2):
            x[0, s, W + a, 0:NB, :] = prev[0, s, a]
    loop(NA, fill, 4)
    for sw in range(SWEEPS):
        for s in range(2):
            for a in (0, PA - 1):
                g[sw, s, a] = jnp.zeros((PB, NC), jnp.float32)
    pl.semaphore_wait(barrier, len(others))
    for s in range(2):
        halo_send((x, 0, 0, 2, W), s)

    @pl.when(node == NODES - 1)
    def _():
        for q in (1, 0, 2):
            start_copy(q).start()

        def own(a):
            for s in range(2):
                start[s, a] = prev[0, s, NA - SLAB + a]
        loop(SLAB, own, 4)

    def sweep(sw, carry):
        e0 = XS * sw
        ex_0 = (x, e0, e0, 2, W)
        exs = [ex_0] + [(x, e0 + k, e0 + k, 1, W) for k in range(1, XS)]
        exs += [(x, e0 + XS, e0 + XS, 2, W)]
        ex_g = (g, sw, LAST + sw, 1, W - 1)
        for s in range(2):
            near_wait(ex_0, s)

        def force(a):
            parts = []
            for s in range(2):
                mid = x[e0, s, W + a]
                total = around(mid)[0:NB] + (
                    x[e0, s, W + a - 1, 0:NB, :] + x[e0, s, W + a + 1, 0:NB, :])
                own = mid[0:NB]
                gap = total - 6.0 * own
                drop[s, a] = ratio[s] * gap
                parts.append((own, jnp.float32(diffusion_values[s]) * gap))
            (u, du), (v, dv) = parts
            uvv = u * v * v
            rate = feed[a]
            return du + (rate * (1.0 - u) - uvv), dv + (uvv - (rate + kill[a]) * v)

        for d in (2, 1, 3, 0):
            def slab(b):
                pair = force(peers[d] * SLAB + b)
                for s in range(2):
                    fsend[sw, s, peers[d], b] = pair[s]
            loop(SLAB, slab, 4)
            if d:
                f_copy(sw, 0, d).start()
        for d in (2, 1, 3):
            f_copy(sw, 1, d).start()

        for s in range(2):
            relay(ex_0, s)

        @pl.when((sw == 0) & (node != NODES - 1))
        def _():
            start_copy(0).wait_recv()

        for s in range(2):
            for d in (1, 3, 2):
                f_copy(sw, s, d).wait_recv()

            def combine(b):
                forces = [fsend[sw, s, node, b]] + [frecv[sw, s, d - 1, b] for d in (1, 2, 3)]
                base = start[s, b]
                for d in range(NODES):
                    total = base
                    for j in range(NODES):
                        total = total + weights[d][j] * forces[j]
                    rsend[sw, s, d, b] = total
            loop(SLAB, combine, 2)
            for d in (2, 1, 3):
                r_copy(sw, s, d).start()

        for s in range(2):
            a_wait(ex_0, s)
        for s in range(2):
            for d in (0, 1, 3, 2):
                if d:
                    r_copy(sw, s, d).wait_recv()
                q = sources[d]

                def right(b):
                    value = rsend[sw, s, 0, b] if d == 0 else rrecv[sw, s, d - 1, b]
                    a = q * SLAB + b
                    g[sw, s, W + a, 0:NB, :] = value * inv[s] - drop[s, a]
                loop(SLAB, right, 4)
            halo_send(ex_g, s)
        for s in range(2):
            relay(ex_g, s)

        for k in range(XS):
            now = ex_g if k == 0 else exs[k]
            for s in range(2):
                b_recv(now, s)
                src, dst = x.at[e0 + k, s], x.at[e0 + k + 1, s]
                for part in (inner, outer):
                    if part is outer:
                        if s == 0 and k > 0:
                            relay(now, 1)
                        if s == 1 and k < XS - 1:
                            relay(exs[k + 1], 0)
                        a_wait(now, s)
                        c_recv(now, s)
                        if k == 0:
                            c_recv(ex_0, s)
                    part(src, t0, sw, s, 1)
                    part(t0, t1, sw, s, 2)
                    part(t1, t0, sw, s, 3)
                    part(t0, dst, sw, s, 4, NB)
                if k < XS - 1:
                    halo_send(exs[k + 1], s)
                else:
                    @pl.when(sw < SWEEPS - 1)
                    def _():
                        halo_send(exs[XS], s)
        return carry
    lax.fori_loop(0, SWEEPS, sweep, 0)

    def drain(a):
        for s in range(2):
            out[0, s, a] = x[LAST, s, W + a, 0:NB, :]
    loop(NA, drain, 4)

    for s in range(2):
        for sw in range(SWEEPS):
            sent((g, sw, LAST + sw, 1, W - 1), s)
            sent((x, XS * sw, XS * sw, 2, W), s)
            for k in range(1, XS):
                sent((x, XS * sw + k, XS * sw + k, 1, W), s)
            for d in (1, 2, 3):
                f_copy(sw, s, d).wait_send()
                r_copy(sw, s, d).wait_send()

    @pl.when(node == NODES - 1)
    def _():
        for q in range(NODES - 1):
            start_copy(q).wait_send()


def body(previous, feed_rate, kill_rate):
    f32 = jnp.float32
    exchanges = LAST + SWEEPS
    dma = pltpu.SemaphoreType.DMA
    return pl.pallas_call(
        kernel,
        out_shape=jax.ShapeDtypeStruct(previous.shape, f32),
        in_specs=[pl.BlockSpec(memory_space=pltpu.VMEM)] * 3,
        out_specs=pl.BlockSpec(memory_space=pltpu.VMEM),
        scratch_shapes=[
            pltpu.VMEM((LAST + 1, 2, PA, PB, NC), f32),
            pltpu.VMEM((SWEEPS, 2, PA, PB, NC), f32),
            pltpu.VMEM((PA, PB, NC), f32),
            pltpu.VMEM((PA, PB, NC), f32),
            pltpu.VMEM((2, NA, NB, NC), f32),
            pltpu.VMEM((SWEEPS, 2, NODES, SLAB, NB, NC), f32),
            pltpu.VMEM((SWEEPS, 2, NODES - 1, SLAB, NB, NC), f32),
            pltpu.VMEM((SWEEPS, 2, NODES, SLAB, NB, NC), f32),
            pltpu.VMEM((SWEEPS, 2, NODES - 1, SLAB, NB, NC), f32),
            pltpu.VMEM((2, SLAB, NB, NC), f32),
            pltpu.VMEM((exchanges, 2, 2, 8, 8, NC), f32),
            pltpu.VMEM((exchanges, 2, 2, 8, 8, NC), f32),
            pltpu.VMEM((exchanges, 2, 4, 2, 8, NC), f32),
            pltpu.VMEM((exchanges, 2, 4, 2, 8, NC), f32),
            pltpu.VMEM((exchanges, 2, W // 2, NB, NC), f32),
            dma((exchanges, 2, 12)), dma((exchanges, 2, 12)),
            dma((SWEEPS, 2, 2, 3)), dma((SWEEPS, 2, 2, 3)),
            dma((3,)), dma((1,)),
        ],
        compiler_params=pltpu.CompilerParams(
            collective_id=0, has_side_effects=True, vmem_limit_bytes=56 * 1024 * 1024),
    )(previous, feed_rate, kill_rate)


def solution(mesh):
    return jax.shard_map(
        body,
        mesh=mesh,
        in_specs=(P("node", None, "sx", "sy", None), P("sx", "sy", None), P("sx", "sy", None)),
        out_specs=P("node", None, "sx", "sy", None),
        check_vma=False,
    )
```

```python
import jax
import jax.numpy as jnp
from jax import lax
from jax.experimental import pallas as pl
from jax.experimental.pallas import tpu as pltpu
from jax.sharding import PartitionSpec as P

SWEEPS = 2
W = 4
NA, NB, NC = 16, 32, 256
PA, PB = NA + 2 * W, NB + 2 * W
NODES = 4
SLAB = NA // NODES
XS = 3
LAST = XS * SWEEPS
MESH = pl.DeviceIdType.MESH

radau_points = [0.088587959512704, 0.409466864440735, 0.787659461760847, 1.0]
time_step = 4.0
diffusion_values = [1.0, 0.5]


def collocation():
    count = len(radau_points)
    table = []
    for row in range(count):
        table.append([0.0] * count)
    for column in range(count):
        poly = [1.0]
        denom = 1.0
        for other in range(count):
            if other != column:
                longer = [0.0] * (len(poly) + 1)
                for place in range(len(poly)):
                    longer[place + 1] = longer[place + 1] + poly[place]
                    longer[place] = longer[place] - radau_points[other] * poly[place]
                poly = longer
                denom = denom * (radau_points[column] - radau_points[other])
        for row in range(count):
            point = radau_points[row]
            total = 0.0
            for place in range(len(poly)):
                total = total + poly[place] * point ** (place + 1) / (place + 1)
            table[row][column] = total / denom
    return table


def chosen(index, values):
    result = jnp.float32(values[-1])
    for place in range(len(values) - 2, -1, -1):
        result = jnp.where(index == place, jnp.float32(values[place]), result)
    return result


def kernel(prev, feed, kill, out, x, g, t0, t1, drop, fsend, frecv, rsend, rrecv, start,
           bsend, brecv, csend, crecv, rbuf, hs, hr, as_, ar, ss, sr):
    node = lax.axis_index("node")
    sx = lax.axis_index("sx")
    sy = lax.axis_index("sy")
    nsx = lax.axis_size("sx")
    nsy = lax.axis_size("sy")
    y = lax.rem(sx, 4)
    edge = [y == 0, y == 3]
    inside = [y != 0, y != 3]
    sx_dev = [lax.rem(sx + nsx - 1, nsx), lax.rem(sx + 1, nsx)]
    in_dev = [lax.rem(sx + 3, nsx), lax.rem(sx + nsx - 3, nsx)]
    out_dev = [lax.rem(sx + nsx - 4, nsx), lax.rem(sx + 4, nsx)]
    sy_dev = [lax.rem(sy + nsy - 1, nsy), lax.rem(sy + 1, nsy)]
    peers = {d: lax.rem(node + d, NODES) for d in range(NODES)}
    sources = {d: lax.rem(node + NODES - d, NODES) for d in range(NODES)}

    qmatrix = collocation()
    coefs = [[time_step * p * d for p in radau_points] for d in diffusion_values]
    inv = [chosen(node, [1.0 / (1.0 + 6.0 * c) for c in cs]) for cs in coefs]
    ratio = [chosen(node, [c / (1.0 + 6.0 * c) for c in cs]) for cs in coefs]
    weights = [[chosen(node, [time_step * qmatrix[(n + d) % NODES][(n - j) % NODES]
                              for n in range(NODES)]) for j in range(NODES)]
               for d in range(NODES)]

    low = lax.broadcasted_iota(jnp.int32, (8, NC), 0) < 4
    barrier = pltpu.get_barrier_semaphore()
    others = [{"node": peers[d]} for d in (1, 2, 3)]
    others += [{"sx": p} for p in sx_dev + in_dev + out_dev] + [{"sy": p} for p in sy_dev]
    others += [{"sx": p, "sy": q} for p in sx_dev for q in sy_dev]
    for other in others:
        pl.semaphore_signal(barrier, inc=1, device_id=other, device_id_type=MESH)

    def loop(count, fn, unroll=1):
        def step(i, carry):
            for k in range(unroll):
                fn(i * unroll + k)
            return carry
        lax.fori_loop(0, count // unroll, step, 0)

    def remote(src, dst, e, s, slot, device):
        return pltpu.make_async_remote_copy(
            src_ref=src, dst_ref=dst, send_sem=hs.at[e, s, slot], recv_sem=hr.at[e, s, slot],
            device_id=device, device_id_type=MESH)

    def span(way, first, last):
        if way == 0:
            return W + first - 1, W + NA + first - 1, last - first + 1
        return W + NA - last, W - last, last - first + 1

    def relayed(ex):
        return 2

    def a_copy(ex, s, way, first, last, slot):
        ref, at, e = ex[:3]
        src, dst, count = span(way, first, last)
        return remote(ref.at[at, s, pl.ds(src, count), pl.ds(0, NB), :],
                      ref.at[at, s, pl.ds(dst, count), pl.ds(0, NB), :],
                      e, s, slot + way, {"sx": sx_dev[way]})

    def relay_in(ex, s, way):
        ref, at, e, first, last = ex
        src, dst, count = span(way, last - relayed(ex) + 1, last)
        return remote(ref.at[at, s, pl.ds(src, count), pl.ds(0, NB), :],
                      rbuf.at[e, s, pl.ds(0, count)], e, s, 2, {"sx": in_dev[way]})

    def relay_out(ex, s, way):
        ref, at, e, first, last = ex
        src, dst, count = span(way, last - relayed(ex) + 1, last)
        return remote(rbuf.at[e, s, pl.ds(0, count)],
                      ref.at[at, s, pl.ds(dst, count), pl.ds(0, NB), :],
                      e, s, 3, {"sx": out_dev[way]})

    def whole(ex, s, way):
        return a_copy(ex, s, way, ex[3], ex[4], 0)

    def direct(ex, s, way):
        return a_copy(ex, s, way, ex[3], ex[4] - relayed(ex), 0)

    def layer(ex, s, way):
        return a_copy(ex, s, way, 1, 1, 10)

    def b_copy(ex, s, way):
        e = ex[2]
        return remote(bsend.at[e, s, way], brecv.at[e, s, way],
                      e, s, 4 + way, {"sy": sy_dev[way]})

    def c_copy(ex, s, n):
        e = ex[2]
        return remote(csend.at[e, s, n], crecv.at[e, s, n],
                      e, s, 6 + n, {"sx": sx_dev[n // 2], "sy": sy_dev[n % 2]})

    def swap(tile):
        return pltpu.roll(tile, 4, 0)

    def first_rows(ex, s, one, two):
        ref, at = ex[:2]
        return jnp.where(low, ref[at, s, one, 0:8, :], swap(ref[at, s, two, 0:8, :]))

    def last_rows(ex, s, one, two):
        ref, at = ex[:2]
        return jnp.where(low, swap(ref[at, s, one, NB - 8:NB, :]), ref[at, s, two, NB - 8:NB, :])

    def put_rows(ex, s, one, two, above, below):
        ref, at = ex[:2]
        ref[at, s, one, NB:PB, :] = jnp.where(low, above, swap(below))
        ref[at, s, two, NB:PB, :] = jnp.where(low, swap(above), below)

    def b_send(ex, s):
        e = ex[2]

        def pack(p):
            bsend[e, s, 0, p] = first_rows(ex, s, W + p, W + 8 + p)
            bsend[e, s, 1, p] = last_rows(ex, s, W + p, W + 8 + p)
        loop(8, pack, 4)
        for way in range(2):
            b_copy(ex, s, way).start()

    def b_recv(ex, s):
        e = ex[2]
        for way in range(2):
            b_copy(ex, s, way).wait_recv()

        def unpack(p):
            put_rows(ex, s, W + p, W + 8 + p, brecv[e, s, 0, p], brecv[e, s, 1, p])
        loop(8, unpack, 4)

    def c_send(ex, s):
        e = ex[2]
        for n in range(4):
            base = W if n < 2 else NA
            for p in range(2):
                rows = first_rows if n % 2 == 0 else last_rows
                csend[e, s, n, p] = rows(ex, s, base + p, base + p + 2)
            c_copy(ex, s, n).start()

    def c_recv(ex, s):
        e = ex[2]
        for n in range(4):
            c_copy(ex, s, n).wait_recv()
        for way in range(2):
            base = W + NA if way == 0 else 0
            for p in range(2):
                put_rows(ex, s, base + p, base + p + 2,
                         crecv[e, s, 2 * way, p], crecv[e, s, 2 * way + 1, p])

    def relay(ex, s):
        for way in range(2):
            @pl.when(edge[1 - way])
            def _():
                relay_in(ex, s, way).wait_recv()
                relay_out(ex, s, way).start()

    def halo_send(ex, s):
        if ex[3] > 1:
            for way in range(2):
                layer(ex, s, way).start()
            b_send(ex, s)
        for way in range(2):
            @pl.when(edge[way])
            def _():
                relay_in(ex, s, way).start()
                direct(ex, s, way).start()

            @pl.when(inside[way])
            def _():
                whole(ex, s, way).start()
        c_send(ex, s)
        if ex[3] == 1:
            b_send(ex, s)

    def near_wait(ex, s):
        for way in range(2):
            layer(ex, s, way).wait_recv()
        b_recv(ex, s)

    def a_wait(ex, s):
        for way in range(2):
            @pl.when(edge[1 - way])
            def _():
                direct(ex, s, way).wait_recv()
                relay_out(ex, s, way).wait_recv()

            @pl.when(inside[1 - way])
            def _():
                whole(ex, s, way).wait_recv()

    def sent(ex, s):
        for way in range(2):
            if ex[3] > 1:
                layer(ex, s, way).wait_send()

            @pl.when(edge[way])
            def _():
                relay_in(ex, s, way).wait_send()
                direct(ex, s, way).wait_send()

            @pl.when(inside[way])
            def _():
                whole(ex, s, way).wait_send()

            @pl.when(edge[1 - way])
            def _():
                relay_out(ex, s, way).wait_send()
        for way in range(2):
            b_copy(ex, s, way).wait_send()
        for n in range(4):
            c_copy(ex, s, n).wait_send()

    def f_copy(sw, s, d):
        return pltpu.make_async_remote_copy(
            src_ref=fsend.at[sw, s, peers[d]], dst_ref=frecv.at[sw, s, d - 1],
            send_sem=as_.at[sw, s, 0, d - 1], recv_sem=ar.at[sw, s, 0, d - 1],
            device_id={"node": peers[d]}, device_id_type=MESH)

    def r_copy(sw, s, d):
        return pltpu.make_async_remote_copy(
            src_ref=rsend.at[sw, s, d], dst_ref=rrecv.at[sw, s, d - 1],
            send_sem=as_.at[sw, s, 1, d - 1], recv_sem=ar.at[sw, s, 1, d - 1],
            device_id={"node": peers[d]}, device_id_type=MESH)

    def start_copy(q):
        return pltpu.make_async_remote_copy(
            src_ref=prev.at[0, :, pl.ds(SLAB * q, SLAB)], dst_ref=start,
            send_sem=ss.at[q], recv_sem=sr.at[0],
            device_id={"node": q}, device_id_type=MESH)

    def around(field):
        total = pltpu.roll(field, 1, 0) + pltpu.roll(field, PB - 1, 0)
        return total + (pltpu.roll(field, 1, 1) + pltpu.roll(field, NC - 1, 1))

    def advance(src, dst, sw, s, base, groups, rows):
        held = {}
        for first, count in groups:
            for a in range(first - 1, first + count + 1):
                if a not in held:
                    held[a] = src[base + a]
        sides = {a: around(held[a])[0:rows] for first, count in groups
                 for a in range(first, first + count)}
        for a, side in sides.items():
            total = side + (held[a - 1][0:rows] + held[a + 1][0:rows])
            dst[base + a, 0:rows, :] = g[sw, s, base + a, 0:rows, :] + ratio[s] * total

    def inner(src, dst, sw, s, level, rows=PB):
        half = NA // 2 - level

        def step(i, carry):
            advance(src, dst, sw, s, W + level + i * half, [(0, half)], rows)
            return carry
        lax.fori_loop(0, 2, step, 0)

    def outer(src, dst, sw, s, level, rows=PB):
        advance(src, dst, sw, s, 0, [(level, W), (PA - W - level, W)], rows)

    def fill(a):
        for s in range(2):
            x[0, s, W + a, 0:NB, :] = prev[0, s, a]
    loop(NA, fill, 4)
    for sw in range(SWEEPS):
        for s in range(2):
            for a in (0, PA - 1):
                g[sw, s, a] = jnp.zeros((PB, NC), jnp.float32)
    pl.semaphore_wait(barrier, len(others))
    for s in range(2):
        halo_send((x, 0, 0, 2, W), s)

    @pl.when(node == NODES - 1)
    def _():
        for q in (1, 0, 2):
            start_copy(q).start()

        def own(a):
            for s in range(2):
                start[s, a] = prev[0, s, NA - SLAB + a]
        loop(SLAB, own, 4)

    def sweep(sw, carry):
        e0 = XS * sw
        ex_0 = (x, e0, e0, 2, W)
        exs = [ex_0] + [(x, e0 + k, e0 + k, 1, W) for k in range(1, XS)]
        exs += [(x, e0 + XS, e0 + XS, 2, W)]
        ex_g = (g, sw, LAST + sw, 1, W - 1)
        for s in range(2):
            near_wait(ex_0, s)

        def force(a):
            parts = []
            for s in range(2):
                mid = x[e0, s, W + a]
                total = around(mid)[0:NB] + (
                    x[e0, s, W + a - 1, 0:NB, :] + x[e0, s, W + a + 1, 0:NB, :])
                own = mid[0:NB]
                gap = total - 6.0 * own
                drop[s, a] = ratio[s] * gap
                parts.append((own, jnp.float32(diffusion_values[s]) * gap))
            (u, du), (v, dv) = parts
            uvv = u * v * v
            rate = feed[a]
            return du + (rate * (1.0 - u) - uvv), dv + (uvv - (rate + kill[a]) * v)

        for d in (2, 1, 3, 0):
            def slab(b):
                pair = force(peers[d] * SLAB + b)
                for s in range(2):
                    fsend[sw, s, peers[d], b] = pair[s]
            loop(SLAB, slab, 4)
            if d:
                f_copy(sw, 0, d).start()
        for d in (2, 1, 3):
            f_copy(sw, 1, d).start()

        for s in range(2):
            relay(ex_0, s)

        @pl.when((sw == 0) & (node != NODES - 1))
        def _():
            start_copy(0).wait_recv()

        for s in range(2):
            for d in (1, 3, 2):
                f_copy(sw, s, d).wait_recv()

            def combine(b):
                forces = [fsend[sw, s, node, b]] + [frecv[sw, s, d - 1, b] for d in (1, 2, 3)]
                base = start[s, b]
                for d in range(NODES):
                    total = base
                    for j in range(NODES):
                        total = total + weights[d][j] * forces[j]
                    rsend[sw, s, d, b] = total
            loop(SLAB, combine, 2)
            for d in (2, 1, 3):
                r_copy(sw, s, d).start()

        for s in range(2):
            a_wait(ex_0, s)
        for s in range(2):
            for d in (0, 1, 3, 2):
                if d:
                    r_copy(sw, s, d).wait_recv()
                q = sources[d]

                def right(b):
                    value = rsend[sw, s, 0, b] if d == 0 else rrecv[sw, s, d - 1, b]
                    a = q * SLAB + b
                    g[sw, s, W + a, 0:NB, :] = value * inv[s] - drop[s, a]
                loop(SLAB, right, 4)
            halo_send(ex_g, s)
            if s == 0:
                relay(ex_g, 0)

        for k in range(XS):
            now = ex_g if k == 0 else exs[k]
            for s in range(2):
                b_recv(now, s)
                src, dst = x.at[e0 + k, s], x.at[e0 + k + 1, s]
                for part in (inner, outer):
                    if part is outer:
                        if s == 0:
                            relay(now, 1)
                        if s == 1 and k < XS - 1:
                            relay(exs[k + 1], 0)
                        a_wait(now, s)
                        c_recv(now, s)
                        if k == 0:
                            c_recv(ex_0, s)
                    part(src, t0, sw, s, 1)
                    part(t0, t1, sw, s, 2)
                    part(t1, t0, sw, s, 3)
                    part(t0, dst, sw, s, 4, NB)
                if k < XS - 1:
                    halo_send(exs[k + 1], s)
                else:
                    @pl.when(sw < SWEEPS - 1)
                    def _():
                        halo_send(exs[XS], s)
        return carry
    lax.fori_loop(0, SWEEPS, sweep, 0)

    def drain(a):
        for s in range(2):
            out[0, s, a] = x[LAST, s, W + a, 0:NB, :]
    loop(NA, drain, 4)

    for s in range(2):
        for sw in range(SWEEPS):
            sent((g, sw, LAST + sw, 1, W - 1), s)
            sent((x, XS * sw, XS * sw, 2, W), s)
            for k in range(1, XS):
                sent((x, XS * sw + k, XS * sw + k, 1, W), s)
            for d in (1, 2, 3):
                f_copy(sw, s, d).wait_send()
                r_copy(sw, s, d).wait_send()

    @pl.when(node == NODES - 1)
    def _():
        for q in range(NODES - 1):
            start_copy(q).wait_send()


def body(previous, feed_rate, kill_rate):
    f32 = jnp.float32
    exchanges = LAST + SWEEPS
    dma = pltpu.SemaphoreType.DMA
    return pl.pallas_call(
        kernel,
        out_shape=jax.ShapeDtypeStruct(previous.shape, f32),
        in_specs=[pl.BlockSpec(memory_space=pltpu.VMEM)] * 3,
        out_specs=pl.BlockSpec(memory_space=pltpu.VMEM),
        scratch_shapes=[
            pltpu.VMEM((LAST + 1, 2, PA, PB, NC), f32),
            pltpu.VMEM((SWEEPS, 2, PA, PB, NC), f32),
            pltpu.VMEM((PA, PB, NC), f32),
            pltpu.VMEM((PA, PB, NC), f32),
            pltpu.VMEM((2, NA, NB, NC), f32),
            pltpu.VMEM((SWEEPS, 2, NODES, SLAB, NB, NC), f32),
            pltpu.VMEM((SWEEPS, 2, NODES - 1, SLAB, NB, NC), f32),
            pltpu.VMEM((SWEEPS, 2, NODES, SLAB, NB, NC), f32),
            pltpu.VMEM((SWEEPS, 2, NODES - 1, SLAB, NB, NC), f32),
            pltpu.VMEM((2, SLAB, NB, NC), f32),
            pltpu.VMEM((exchanges, 2, 2, 8, 8, NC), f32),
            pltpu.VMEM((exchanges, 2, 2, 8, 8, NC), f32),
            pltpu.VMEM((exchanges, 2, 4, 2, 8, NC), f32),
            pltpu.VMEM((exchanges, 2, 4, 2, 8, NC), f32),
            pltpu.VMEM((exchanges, 2, W // 2, NB, NC), f32),
            dma((exchanges, 2, 12)), dma((exchanges, 2, 12)),
            dma((SWEEPS, 2, 2, 3)), dma((SWEEPS, 2, 2, 3)),
            dma((3,)), dma((1,)),
        ],
        compiler_params=pltpu.CompilerParams(
            collective_id=0, has_side_effects=True, vmem_limit_bytes=56 * 1024 * 1024),
    )(previous, feed_rate, kill_rate)


def solution(mesh):
    return jax.shard_map(
        body,
        mesh=mesh,
        in_specs=(P("node", None, "sx", "sy", None), P("sx", "sy", None), P("sx", "sy", None)),
        out_specs=P("node", None, "sx", "sy", None),
        check_vma=False,
    )
```

```python
import jax
import jax.numpy as jnp
from jax import lax
from jax.experimental import pallas as pl
from jax.experimental.pallas import tpu as pltpu
from jax.sharding import PartitionSpec as P

SWEEPS = 2
W = 4
NA, NB, NC = 16, 32, 256
PA, PB = NA + 2 * W, NB + 2 * W
NODES = 4
SLAB = NA // NODES
XS = 3
LAST = XS * SWEEPS
MESH = pl.DeviceIdType.MESH

radau_points = [0.088587959512704, 0.409466864440735, 0.787659461760847, 1.0]
time_step = 4.0
diffusion_values = [1.0, 0.5]


def collocation():
    count = len(radau_points)
    table = []
    for row in range(count):
        table.append([0.0] * count)
    for column in range(count):
        poly = [1.0]
        denom = 1.0
        for other in range(count):
            if other != column:
                longer = [0.0] * (len(poly) + 1)
                for place in range(len(poly)):
                    longer[place + 1] = longer[place + 1] + poly[place]
                    longer[place] = longer[place] - radau_points[other] * poly[place]
                poly = longer
                denom = denom * (radau_points[column] - radau_points[other])
        for row in range(count):
            point = radau_points[row]
            total = 0.0
            for place in range(len(poly)):
                total = total + poly[place] * point ** (place + 1) / (place + 1)
            table[row][column] = total / denom
    return table


def chosen(index, values):
    result = jnp.float32(values[-1])
    for place in range(len(values) - 2, -1, -1):
        result = jnp.where(index == place, jnp.float32(values[place]), result)
    return result


def kernel(prev, feed, kill, out, x, g, t0, t1, drop, fsend, frecv, rsend, rrecv, start,
           bsend, brecv, csend, crecv, rbuf, hs, hr, as_, ar, ss, sr):
    node = lax.axis_index("node")
    sx = lax.axis_index("sx")
    sy = lax.axis_index("sy")
    nsx = lax.axis_size("sx")
    nsy = lax.axis_size("sy")
    y = lax.rem(sx, 4)
    edge = [y == 0, y == 3]
    inside = [y != 0, y != 3]
    sx_dev = [lax.rem(sx + nsx - 1, nsx), lax.rem(sx + 1, nsx)]
    in_dev = [lax.rem(sx + 3, nsx), lax.rem(sx + nsx - 3, nsx)]
    out_dev = [lax.rem(sx + nsx - 4, nsx), lax.rem(sx + 4, nsx)]
    sy_dev = [lax.rem(sy + nsy - 1, nsy), lax.rem(sy + 1, nsy)]
    peers = {d: lax.rem(node + d, NODES) for d in range(NODES)}
    sources = {d: lax.rem(node + NODES - d, NODES) for d in range(NODES)}

    qmatrix = collocation()
    coefs = [[time_step * p * d for p in radau_points] for d in diffusion_values]
    inv = [chosen(node, [1.0 / (1.0 + 6.0 * c) for c in cs]) for cs in coefs]
    ratio = [chosen(node, [c / (1.0 + 6.0 * c) for c in cs]) for cs in coefs]
    weights = [[chosen(node, [time_step * qmatrix[(n + d) % NODES][(n - j) % NODES]
                              for n in range(NODES)]) for j in range(NODES)]
               for d in range(NODES)]

    low = lax.broadcasted_iota(jnp.int32, (8, NC), 0) < 4
    barrier = pltpu.get_barrier_semaphore()
    others = [{"node": peers[d]} for d in (1, 2, 3)]
    others += [{"sx": p} for p in sx_dev + in_dev + out_dev] + [{"sy": p} for p in sy_dev]
    others += [{"sx": p, "sy": q} for p in sx_dev for q in sy_dev]
    for other in others:
        pl.semaphore_signal(barrier, inc=1, device_id=other, device_id_type=MESH)

    def loop(count, fn, unroll=1):
        def step(i, carry):
            for k in range(unroll):
                fn(i * unroll + k)
            return carry
        lax.fori_loop(0, count // unroll, step, 0)

    def remote(src, dst, e, s, slot, device):
        return pltpu.make_async_remote_copy(
            src_ref=src, dst_ref=dst, send_sem=hs.at[e, s, slot], recv_sem=hr.at[e, s, slot],
            device_id=device, device_id_type=MESH)

    def span(way, first, last):
        if way == 0:
            return W + first - 1, W + NA + first - 1, last - first + 1
        return W + NA - last, W - last, last - first + 1

    def relayed(ex):
        return 2

    def a_copy(ex, s, way, first, last, slot):
        ref, at, e = ex[:3]
        src, dst, count = span(way, first, last)
        return remote(ref.at[at, s, pl.ds(src, count), pl.ds(0, NB), :],
                      ref.at[at, s, pl.ds(dst, count), pl.ds(0, NB), :],
                      e, s, slot + way, {"sx": sx_dev[way]})

    def relay_in(ex, s, way):
        ref, at, e, first, last = ex
        src, dst, count = span(way, last - relayed(ex) + 1, last)
        return remote(ref.at[at, s, pl.ds(src, count), pl.ds(0, NB), :],
                      rbuf.at[e, s, pl.ds(0, count)], e, s, 2, {"sx": in_dev[way]})

    def relay_out(ex, s, way):
        ref, at, e, first, last = ex
        src, dst, count = span(way, last - relayed(ex) + 1, last)
        return remote(rbuf.at[e, s, pl.ds(0, count)],
                      ref.at[at, s, pl.ds(dst, count), pl.ds(0, NB), :],
                      e, s, 3, {"sx": out_dev[way]})

    def whole(ex, s, way):
        return a_copy(ex, s, way, ex[3], ex[4], 0)

    def direct(ex, s, way):
        return a_copy(ex, s, way, ex[3], ex[4] - relayed(ex), 0)

    def layer(ex, s, way):
        return a_copy(ex, s, way, 1, 1, 10)

    def b_copy(ex, s, way):
        e = ex[2]
        return remote(bsend.at[e, s, way], brecv.at[e, s, way],
                      e, s, 4 + way, {"sy": sy_dev[way]})

    def c_copy(ex, s, n):
        e = ex[2]
        return remote(csend.at[e, s, n], crecv.at[e, s, n],
                      e, s, 6 + n, {"sx": sx_dev[n // 2], "sy": sy_dev[n % 2]})

    def swap(tile):
        return pltpu.roll(tile, 4, 0)

    def first_rows(ex, s, one, two):
        ref, at = ex[:2]
        return jnp.where(low, ref[at, s, one, 0:8, :], swap(ref[at, s, two, 0:8, :]))

    def last_rows(ex, s, one, two):
        ref, at = ex[:2]
        return jnp.where(low, swap(ref[at, s, one, NB - 8:NB, :]), ref[at, s, two, NB - 8:NB, :])

    def put_rows(ex, s, one, two, above, below):
        ref, at = ex[:2]
        ref[at, s, one, NB:PB, :] = jnp.where(low, above, swap(below))
        ref[at, s, two, NB:PB, :] = jnp.where(low, swap(above), below)

    def b_send(ex, s):
        e = ex[2]

        def pack(p):
            bsend[e, s, 0, p] = first_rows(ex, s, W + p, W + 8 + p)
            bsend[e, s, 1, p] = last_rows(ex, s, W + p, W + 8 + p)
        loop(8, pack, 4)
        for way in range(2):
            b_copy(ex, s, way).start()

    def b_recv(ex, s):
        e = ex[2]
        for way in range(2):
            b_copy(ex, s, way).wait_recv()

        def unpack(p):
            put_rows(ex, s, W + p, W + 8 + p, brecv[e, s, 0, p], brecv[e, s, 1, p])
        loop(8, unpack, 4)

    def c_send(ex, s):
        e = ex[2]
        for n in range(4):
            base = W if n < 2 else NA
            for p in range(2):
                rows = first_rows if n % 2 == 0 else last_rows
                csend[e, s, n, p] = rows(ex, s, base + p, base + p + 2)
            c_copy(ex, s, n).start()

    def c_recv(ex, s):
        e = ex[2]
        for n in range(4):
            c_copy(ex, s, n).wait_recv()
        for way in range(2):
            base = W + NA if way == 0 else 0
            for p in range(2):
                put_rows(ex, s, base + p, base + p + 2,
                         crecv[e, s, 2 * way, p], crecv[e, s, 2 * way + 1, p])

    def relay(ex, s):
        for way in range(2):
            @pl.when(edge[1 - way])
            def _():
                relay_in(ex, s, way).wait_recv()
                relay_out(ex, s, way).start()

    def halo_send(ex, s):
        if ex[3] > 1:
            for way in range(2):
                layer(ex, s, way).start()
            b_send(ex, s)
        for way in range(2):
            @pl.when(edge[way])
            def _():
                relay_in(ex, s, way).start()
                direct(ex, s, way).start()

            @pl.when(inside[way])
            def _():
                whole(ex, s, way).start()
        if ex[3] == 1:
            b_send(ex, s)
        c_send(ex, s)

    def near_wait(ex, s):
        for way in range(2):
            layer(ex, s, way).wait_recv()
        b_recv(ex, s)

    def a_wait(ex, s):
        for way in range(2):
            @pl.when(edge[1 - way])
            def _():
                direct(ex, s, way).wait_recv()
                relay_out(ex, s, way).wait_recv()

            @pl.when(inside[1 - way])
            def _():
                whole(ex, s, way).wait_recv()

    def sent(ex, s):
        for way in range(2):
            if ex[3] > 1:
                layer(ex, s, way).wait_send()

            @pl.when(edge[way])
            def _():
                relay_in(ex, s, way).wait_send()
                direct(ex, s, way).wait_send()

            @pl.when(inside[way])
            def _():
                whole(ex, s, way).wait_send()

            @pl.when(edge[1 - way])
            def _():
                relay_out(ex, s, way).wait_send()
        for way in range(2):
            b_copy(ex, s, way).wait_send()
        for n in range(4):
            c_copy(ex, s, n).wait_send()

    def f_copy(sw, s, d):
        return pltpu.make_async_remote_copy(
            src_ref=fsend.at[sw, s, peers[d]], dst_ref=frecv.at[sw, s, d - 1],
            send_sem=as_.at[sw, s, 0, d - 1], recv_sem=ar.at[sw, s, 0, d - 1],
            device_id={"node": peers[d]}, device_id_type=MESH)

    def r_copy(sw, s, d):
        return pltpu.make_async_remote_copy(
            src_ref=rsend.at[sw, s, d], dst_ref=rrecv.at[sw, s, d - 1],
            send_sem=as_.at[sw, s, 1, d - 1], recv_sem=ar.at[sw, s, 1, d - 1],
            device_id={"node": peers[d]}, device_id_type=MESH)

    def start_copy(q):
        return pltpu.make_async_remote_copy(
            src_ref=prev.at[0, :, pl.ds(SLAB * q, SLAB)], dst_ref=start,
            send_sem=ss.at[q], recv_sem=sr.at[0],
            device_id={"node": q}, device_id_type=MESH)

    def around(field):
        total = pltpu.roll(field, 1, 0) + pltpu.roll(field, PB - 1, 0)
        return total + (pltpu.roll(field, 1, 1) + pltpu.roll(field, NC - 1, 1))

    def advance(src, dst, sw, s, base, groups, rows):
        held = {}
        for first, count in groups:
            for a in range(first - 1, first + count + 1):
                if a not in held:
                    held[a] = src[base + a]
        sides = {a: around(held[a])[0:rows] for first, count in groups
                 for a in range(first, first + count)}
        for a, side in sides.items():
            total = side + (held[a - 1][0:rows] + held[a + 1][0:rows])
            dst[base + a, 0:rows, :] = g[sw, s, base + a, 0:rows, :] + ratio[s] * total

    def inner(src, dst, sw, s, level, rows=PB):
        half = NA // 2 - level

        def step(i, carry):
            advance(src, dst, sw, s, W + level + i * half, [(0, half)], rows)
            return carry
        lax.fori_loop(0, 2, step, 0)

    def outer(src, dst, sw, s, level, rows=PB):
        advance(src, dst, sw, s, 0, [(level, W), (PA - W - level, W)], rows)

    def fill(a):
        for s in range(2):
            x[0, s, W + a, 0:NB, :] = prev[0, s, a]
    loop(NA, fill, 4)
    for sw in range(SWEEPS):
        for s in range(2):
            for a in (0, PA - 1):
                g[sw, s, a] = jnp.zeros((PB, NC), jnp.float32)
    pl.semaphore_wait(barrier, len(others))
    for s in range(2):
        halo_send((x, 0, 0, 2, W), s)

    @pl.when(node == NODES - 1)
    def _():
        for q in (1, 0, 2):
            start_copy(q).start()

        def own(a):
            for s in range(2):
                start[s, a] = prev[0, s, NA - SLAB + a]
        loop(SLAB, own, 4)

    def sweep(sw, carry):
        e0 = XS * sw
        ex_0 = (x, e0, e0, 2, W)
        exs = [ex_0] + [(x, e0 + k, e0 + k, 1, W) for k in range(1, XS)]
        exs += [(x, e0 + XS, e0 + XS, 2, W)]
        ex_g = (g, sw, LAST + sw, 1, W - 1)
        for s in range(2):
            near_wait(ex_0, s)

        def force(a):
            parts = []
            for s in range(2):
                mid = x[e0, s, W + a]
                total = around(mid)[0:NB] + (
                    x[e0, s, W + a - 1, 0:NB, :] + x[e0, s, W + a + 1, 0:NB, :])
                own = mid[0:NB]
                gap = total - 6.0 * own
                drop[s, a] = ratio[s] * gap
                parts.append((own, jnp.float32(diffusion_values[s]) * gap))
            (u, du), (v, dv) = parts
            uvv = u * v * v
            rate = feed[a]
            return du + (rate * (1.0 - u) - uvv), dv + (uvv - (rate + kill[a]) * v)

        for d in (2, 1, 3, 0):
            def slab(b):
                pair = force(peers[d] * SLAB + b)
                for s in range(2):
                    fsend[sw, s, peers[d], b] = pair[s]
            loop(SLAB, slab, 4)
            if d:
                f_copy(sw, 0, d).start()
        for d in (2, 1, 3):
            f_copy(sw, 1, d).start()

        for s in range(2):
            relay(ex_0, s)

        @pl.when((sw == 0) & (node != NODES - 1))
        def _():
            start_copy(0).wait_recv()

        for s in range(2):
            for d in (1, 3, 2):
                f_copy(sw, s, d).wait_recv()

            def combine(b):
                forces = [fsend[sw, s, node, b]] + [frecv[sw, s, d - 1, b] for d in (1, 2, 3)]
                base = start[s, b]
                for d in range(NODES):
                    total = base
                    for j in range(NODES):
                        total = total + weights[d][j] * forces[j]
                    rsend[sw, s, d, b] = total
            loop(SLAB, combine, 4)
            for d in (2, 1, 3):
                r_copy(sw, s, d).start()

        for s in range(2):
            a_wait(ex_0, s)
        for s in range(2):
            for d in (0, 1, 3, 2):
                if d:
                    r_copy(sw, s, d).wait_recv()
                q = sources[d]

                def right(b):
                    value = rsend[sw, s, 0, b] if d == 0 else rrecv[sw, s, d - 1, b]
                    a = q * SLAB + b
                    g[sw, s, W + a, 0:NB, :] = value * inv[s] - drop[s, a]
                loop(SLAB, right, 4)
            halo_send(ex_g, s)
            if s == 0:
                relay(ex_g, 0)

        for k in range(XS):
            now = ex_g if k == 0 else exs[k]
            for s in range(2):
                b_recv(now, s)
                src, dst = x.at[e0 + k, s], x.at[e0 + k + 1, s]
                for part in (inner, outer):
                    if part is outer:
                        if s == 0:
                            relay(now, 1)
                        if s == 1 and k < XS - 1:
                            relay(exs[k + 1], 0)
                        a_wait(now, s)
                        c_recv(now, s)
                        if k == 0:
                            c_recv(ex_0, s)
                    part(src, t0, sw, s, 1)
                    part(t0, t1, sw, s, 2)
                    part(t1, t0, sw, s, 3)
                    part(t0, dst, sw, s, 4, NB)
                if k < XS - 1:
                    halo_send(exs[k + 1], s)
                else:
                    @pl.when(sw < SWEEPS - 1)
                    def _():
                        halo_send(exs[XS], s)
        return carry
    lax.fori_loop(0, SWEEPS, sweep, 0)

    def drain(a):
        for s in range(2):
            out[0, s, a] = x[LAST, s, W + a, 0:NB, :]
    loop(NA, drain, 4)

    for s in range(2):
        for sw in range(SWEEPS):
            sent((g, sw, LAST + sw, 1, W - 1), s)
            sent((x, XS * sw, XS * sw, 2, W), s)
            for k in range(1, XS):
                sent((x, XS * sw + k, XS * sw + k, 1, W), s)
            for d in (1, 2, 3):
                f_copy(sw, s, d).wait_send()
                r_copy(sw, s, d).wait_send()

    @pl.when(node == NODES - 1)
    def _():
        for q in range(NODES - 1):
            start_copy(q).wait_send()


def body(previous, feed_rate, kill_rate):
    f32 = jnp.float32
    exchanges = LAST + SWEEPS
    dma = pltpu.SemaphoreType.DMA
    return pl.pallas_call(
        kernel,
        out_shape=jax.ShapeDtypeStruct(previous.shape, f32),
        in_specs=[pl.BlockSpec(memory_space=pltpu.VMEM)] * 3,
        out_specs=pl.BlockSpec(memory_space=pltpu.VMEM),
        scratch_shapes=[
            pltpu.VMEM((LAST + 1, 2, PA, PB, NC), f32),
            pltpu.VMEM((SWEEPS, 2, PA, PB, NC), f32),
            pltpu.VMEM((PA, PB, NC), f32),
            pltpu.VMEM((PA, PB, NC), f32),
            pltpu.VMEM((2, NA, NB, NC), f32),
            pltpu.VMEM((SWEEPS, 2, NODES, SLAB, NB, NC), f32),
            pltpu.VMEM((SWEEPS, 2, NODES - 1, SLAB, NB, NC), f32),
            pltpu.VMEM((SWEEPS, 2, NODES, SLAB, NB, NC), f32),
            pltpu.VMEM((SWEEPS, 2, NODES - 1, SLAB, NB, NC), f32),
            pltpu.VMEM((2, SLAB, NB, NC), f32),
            pltpu.VMEM((exchanges, 2, 2, 8, 8, NC), f32),
            pltpu.VMEM((exchanges, 2, 2, 8, 8, NC), f32),
            pltpu.VMEM((exchanges, 2, 4, 2, 8, NC), f32),
            pltpu.VMEM((exchanges, 2, 4, 2, 8, NC), f32),
            pltpu.VMEM((exchanges, 2, W // 2, NB, NC), f32),
            dma((exchanges, 2, 12)), dma((exchanges, 2, 12)),
            dma((SWEEPS, 2, 2, 3)), dma((SWEEPS, 2, 2, 3)),
            dma((3,)), dma((1,)),
        ],
        compiler_params=pltpu.CompilerParams(
            collective_id=0, has_side_effects=True, vmem_limit_bytes=56 * 1024 * 1024),
    )(previous, feed_rate, kill_rate)


def solution(mesh):
    return jax.shard_map(
        body,
        mesh=mesh,
        in_specs=(P("node", None, "sx", "sy", None), P("sx", "sy", None), P("sx", "sy", None)),
        out_specs=P("node", None, "sx", "sy", None),
        check_vma=False,
    )
```
